8 devices in a mesh: dp: 1 (over z), tp: 2 (over y), pp: 4 (over x, core).
Axes of the slice: x: 2, y: 2, z: 1, core: 2. Of those that a mesh axis runs over, the one named last changes fastest.
Arguments:
- x_in: bfloat16 [8, 6, 512, 1536], P('dp')
- seq_lens: int32 [8, 6], P('dp')
- ln1_gain: bfloat16 [4, 1536], P('pp')
- ln1_shift: bfloat16 [4, 1536], P('pp')
- w_qkv: bfloat16 [4, 1536, 3, 1536], P('pp', None, None, 'tp')
- b_qkv: bfloat16 [4, 3, 16, 96], P('pp', None, 'tp')
- w_out: bfloat16 [4, 1536, 1536], P('pp', 'tp')
- b_out: bfloat16 [4, 1536], P('pp')
- ln2_gain: bfloat16 [4, 1536], P('pp')
- ln2_shift: bfloat16 [4, 1536], P('pp')
- w_up: bfloat16 [4, 1536, 6144], P('pp', None, 'tp')
- b_up: bfloat16 [4, 6144], P('pp', 'tp')
- w_down: bfloat16 [4, 6144, 1536], P('pp', 'tp')
- b_down: bfloat16 [4, 1536], P('pp')
Outputs:
- output: bfloat16 [4, 8, 6, 512, 1536], P('pp', 'dp')
All inputs are finite; a program needn't handle non-finite values.
Results may differ from the reference program's by a relative error of at most 0.0173956.
Values are sent between devices in bfloat16 or wider.
A program may use at most 1 GiB of HBM per device.

```python
import jax
import jax.numpy as jnp
from jax import lax
import math

LAYERS = 4
MICRO_COUNT = 8
BATCH_SIZE = 6
SEQ_LEN = 512
MODEL_DIM = 1536
NUM_HEADS = 16
HIDDEN_DIM = 6144
HEAD_DIM = MODEL_DIM // NUM_HEADS


def alibi_slopes(heads_n):
    closest = 2 ** int(math.floor(math.log2(heads_n)))
    base_rate = 2.0 ** (-8.0 / closest)
    slope_list = [base_rate ** (head_idx + 1) for head_idx in range(closest)]
    extra_rate = 2.0 ** (-4.0 / closest)
    slope_list = slope_list + [extra_rate ** (2 * head_idx + 1) for head_idx in range(min(closest, heads_n - closest))]
    return jnp.array(slope_list, dtype=jnp.float32)


def layer_norm(values, gain_vec, shift_vec):
    val_f = values.astype(jnp.float32)
    mean_val = jnp.mean(val_f, axis=-1, keepdims=True)
    centered = val_f - mean_val
    var_val = jnp.mean(centered * centered, axis=-1, keepdims=True)
    normed = centered * lax.rsqrt(var_val + 1e-5)
    return (normed * gain_vec.astype(jnp.float32) + shift_vec.astype(jnp.float32)).astype(jnp.bfloat16)


def attention(query_all, key_all, val_all, slopes, lens_row):
    batch_n, seq_n, heads_n, head_dim = query_all.shape
    blk_len = min(seq_n, 128)
    key_pos = jnp.arange(seq_n)
    key_ok = key_pos[None, :] < lens_row[:, None]
    key_f = key_all.astype(jnp.float32)
    val_f = val_all.astype(jnp.float32)

    def one_block(blk_idx):
        query_blk = lax.dynamic_slice_in_dim(query_all, blk_idx * blk_len, blk_len, 1).astype(jnp.float32)
        scores = jnp.einsum('bqhe,bkhe->bhqk', query_blk, key_f) * (head_dim ** -0.5)
        query_pos = blk_idx * blk_len + jnp.arange(blk_len)
        distance = (query_pos[:, None] - key_pos[None, :]).astype(jnp.float32)
        scores = scores - slopes[None, :, None, None] * distance[None, None]
        allowed = (key_pos[None, :] <= query_pos[:, None])[None, None] & key_ok[:, None, None, :]
        scores = jnp.where(allowed, scores, -1e30)
        prob_bf = jax.nn.softmax(scores, axis=-1).astype(jnp.bfloat16)
        return jnp.einsum('bhqk,bkhe->bqhe', prob_bf.astype(jnp.float32), val_f).astype(jnp.bfloat16)

    blocks = lax.map(one_block, jnp.arange(seq_n // blk_len))
    return jnp.moveaxis(blocks, 0, 1).reshape(batch_n, seq_n, heads_n * head_dim)


def bloom_layer(act_in, lens_row, layer_w, slopes):
    ln1_gain, ln1_shift, w_qkv, b_qkv, w_out, b_out, ln2_gain, ln2_shift, w_up, b_up, w_down, b_down = layer_w
    batch_n, seq_n, model_n = act_in.shape
    tokens_n = batch_n * seq_n
    heads_n, head_dim = b_qkv.shape[1], b_qkv.shape[2]
    flat_in = act_in.reshape(tokens_n, model_n)
    normed = layer_norm(flat_in, ln1_gain, ln1_shift)
    qkv_all = (jnp.dot(normed, w_qkv.reshape(model_n, 3 * model_n), preferred_element_type=jnp.float32) + b_qkv.reshape(3 * model_n).astype(jnp.float32)).astype(jnp.bfloat16)
    qkv_all = qkv_all.reshape(batch_n, seq_n, 3, heads_n, head_dim)
    context = attention(qkv_all[:, :, 0], qkv_all[:, :, 1], qkv_all[:, :, 2], slopes, lens_row)
    attn_out = jnp.dot(context.reshape(tokens_n, model_n), w_out, preferred_element_type=jnp.float32)
    resid_act = (flat_in.astype(jnp.float32) + attn_out + b_out.astype(jnp.float32)).astype(jnp.bfloat16)
    normed_mlp = layer_norm(resid_act, ln2_gain, ln2_shift)
    hidden_act = jax.nn.gelu(jnp.dot(normed_mlp, w_up, preferred_element_type=jnp.float32) + b_up.astype(jnp.float32), approximate=True).astype(jnp.bfloat16)
    mlp_out = jnp.dot(hidden_act, w_down, preferred_element_type=jnp.float32)
    result = (resid_act.astype(jnp.float32) + mlp_out + b_down.astype(jnp.float32)).astype(jnp.bfloat16)
    return result.reshape(batch_n, seq_n, model_n)


def setup_inputs(seed: int = 0, part: int = 0) -> dict:
    w_keys = jax.random.split(jax.random.key(seed), 12)
    part_keys = jax.random.split(jax.random.fold_in(jax.random.key(seed + 1), part), 2)

    def normal_draw(rng_key, arr_shape, std_dev, offset):
        return (offset + std_dev * jax.random.normal(rng_key, arr_shape, jnp.float32)).astype(jnp.bfloat16)

    width_scale = MODEL_DIM ** -0.5
    lens_draw = jax.random.randint(part_keys[1], (MICRO_COUNT, BATCH_SIZE), 1, SEQ_LEN + 1, dtype=jnp.int32)
    return dict(
        x_in=normal_draw(part_keys[0], (MICRO_COUNT, BATCH_SIZE, SEQ_LEN, MODEL_DIM), 1.0, 0.0),
        seq_lens=lens_draw.at[0, 0].set(SEQ_LEN),
        ln1_gain=normal_draw(w_keys[0], (LAYERS, MODEL_DIM), 0.3, 1.0),
        ln1_shift=normal_draw(w_keys[1], (LAYERS, MODEL_DIM), 0.3, 0.0),
        w_qkv=normal_draw(w_keys[2], (LAYERS, MODEL_DIM, 3, MODEL_DIM), width_scale, 0.0),
        b_qkv=normal_draw(w_keys[3], (LAYERS, 3, NUM_HEADS, HEAD_DIM), 0.3, 0.0),
        w_out=normal_draw(w_keys[4], (LAYERS, MODEL_DIM, MODEL_DIM), width_scale, 0.0),
        b_out=normal_draw(w_keys[5], (LAYERS, MODEL_DIM), 0.3, 0.0),
        ln2_gain=normal_draw(w_keys[6], (LAYERS, MODEL_DIM), 0.3, 1.0),
        ln2_shift=normal_draw(w_keys[7], (LAYERS, MODEL_DIM), 0.3, 0.0),
        w_up=normal_draw(w_keys[8], (LAYERS, MODEL_DIM, HIDDEN_DIM), width_scale, 0.0),
        b_up=normal_draw(w_keys[9], (LAYERS, HIDDEN_DIM), 0.3, 0.0),
        w_down=normal_draw(w_keys[10], (LAYERS, HIDDEN_DIM, MODEL_DIM), HIDDEN_DIM ** -0.5, 0.0),
        b_down=normal_draw(w_keys[11], (LAYERS, MODEL_DIM), 0.3, 0.0),
    )


def reference(x_in, seq_lens, ln1_gain, ln1_shift, w_qkv, b_qkv, w_out, b_out, ln2_gain, ln2_shift, w_up, b_up, w_down, b_down):
    slopes = alibi_slopes(NUM_HEADS)

    def layer_step(current, layer_w):
        new_act = lax.map(lambda micro_pair: bloom_layer(micro_pair[0], micro_pair[1], layer_w, slopes), (current, seq_lens))
        return new_act, new_act

    final_act, hidden = lax.scan(layer_step, x_in, (ln1_gain, ln1_shift, w_qkv, b_qkv, w_out, b_out, ln2_gain, ln2_shift, w_up, b_up, w_down, b_down))
    return hidden
```

```python
import functools
import math

import jax
import jax.numpy as jnp
import numpy as np
from jax import lax
from jax.experimental import pallas as pl
from jax.experimental.pallas import tpu as pltpu
from jax.sharding import PartitionSpec as P

MESH = pl.DeviceIdType.MESH
LOG2E = math.log2(math.e)
MASKED = -1e34
F32 = jnp.float32
BF16 = jnp.bfloat16
LN1_G, LN1_S, B_OUT, LN2_G, LN2_S, B_DOWN, B_QKV, B_UP = 0, 2, 4, 6, 8, 10, 12, 15


def alibi_slopes(heads_n):
    closest = 2 ** int(math.floor(math.log2(heads_n)))
    base_rate = 2.0 ** (-8.0 / closest)
    slope_list = [base_rate ** (head_idx + 1) for head_idx in range(closest)]
    extra_rate = 2.0 ** (-4.0 / closest)
    return slope_list + [extra_rate ** (2 * head_idx + 1) for head_idx in range(min(closest, heads_n - closest))]


def normalize(val_f, gain, shift):
    width = val_f.shape[-1]
    mean_val = jnp.sum(val_f, axis=-1, keepdims=True) * (1.0 / width)
    centered = val_f - mean_val
    var_val = jnp.sum(centered * centered, axis=-1, keepdims=True) * (1.0 / width)
    normed = centered * lax.rsqrt(var_val + 1e-5)
    return (normed * gain + shift).astype(BF16)


def row_blocks(rows_n, body, block=16, unroll=8):
    def some(step, carry):
        for k in range(unroll):
            body(pl.ds(pl.multiple_of(step * (block * unroll) + k * block, block), block))
        return carry

    lax.fori_loop(0, rows_n // (block * unroll), some, 0)


def gelu(val):
    inner = val * (0.7978845608028654 + (0.7978845608028654 * 0.044715) * (val * val))
    half = 0.5 * val
    return half + half * jnp.tanh(inner)


def stage_kernel(
    units, head_dim,
    x_hbm, lens, slopes, small_hbm, wqkv, wout, wup, wdown,
    hidden, inbox, ostage, wa_qkv, wa_out, wa_up, wa_down, wb_qkv, wb_out, wb_up, wb_down,
    small, x_buf, a_buf, qkv_buf, ctx_buf, acc, u_buf, bias, score_buf, prob_buf, out_buf, ring,
    small_sem, wa_recv, wb_recv, w_send, w_fwd, in_recv, st_recv, ring_sem, x_sem, l_sem,
    y_send, c_send, x_send, f_send,
):
    dp = lax.axis_index('dp')
    y = lax.axis_index('tp')
    pp = lax.axis_index('pp')
    core = lax.rem(pp, 2)
    chip_x = pp // 2
    odd = lax.rem(chip_x + y, 2)
    stage = 2 * chip_x + odd
    own = core == odd
    not_own = core != odd
    is_odd = odd == 1
    is_even = odd == 0
    partner = (dp, y, 2 * chip_x + 1 - core)
    y_peer = (dp, 1 - y, pp)
    y_store = (dp, 1 - y, 2 * chip_x + 1)
    y_other = (dp, 1 - y, 2 * chip_x + 1 - core)
    x_peer = (dp, y, lax.rem(pp + 2, 4))
    seq_n, width = a_buf.shape
    half_w = wout.shape[0]
    heads_loc = half_w // head_dim
    parts = wup.shape[1] // width
    chunks = 2 * parts

    barrier = pltpu.get_barrier_semaphore()
    for other in (partner, y_peer, y_other, x_peer):
        pl.semaphore_signal(barrier, inc=1, device_id=other, device_id_type=MESH)
    pl.semaphore_wait(barrier, 4)

    def remote(src, dst, send_sem, recv_sem, device):
        return pltpu.make_async_remote_copy(src_ref=src, dst_ref=dst, send_sem=send_sem, recv_sem=recv_sem, device_id=device, device_id_type=MESH)

    def wait_on(ref, sem):
        pltpu.make_async_copy(ref, ref, sem).wait()

    def pieces(qkv, out, up, down, up_cut):
        found = [qkv.at[j] for j in range(3)] + [out]
        for m in range(parts):
            found.append(up.at[:, pl.ds(m * width, width)] if up_cut else up.at[m])
            found.append(down.at[pl.ds(m * width, width), :])
        return found

    mine = pieces(wqkv, wout, wup, wdown, True)
    got_a = pieces(wa_qkv, wa_out, wa_up, wa_down, False)
    got_b = pieces(wb_qkv, wb_out, wb_up, wb_down, False)
    pieces_n = len(mine)

    small_local = pltpu.make_async_copy(small_hbm, small.at[0], small_sem.at[0])
    small_give = remote(small_hbm, small.at[0], small_sem.at[1], small_sem.at[2], partner)
    small_cross = remote(small_hbm, small.at[1], small_sem.at[1], small_sem.at[3], y_peer)
    small_pass = remote(small.at[1], small.at[1], small_sem.at[4], small_sem.at[3], partner)

    @pl.when(own)
    def _():
        small_local.start()
        small_give.start()
        for j in range(pieces_n):
            remote(mine[j], got_a[j], w_send.at[j], wa_recv.at[j], partner).start()

    @pl.when(not_own)
    def _():
        small_cross.start()
        for j in range(pieces_n):
            remote(mine[j], got_b[j], w_send.at[j], wb_recv.at[j], y_peer).start()

    def pass_on(j):
        return remote(got_b[j], got_b[j], w_fwd.at[j], wb_recv.at[j], partner)

    def arrive_a(j):
        pl.when(not_own)(lambda: wait_on(got_a[j], wa_recv.at[j]))

    def arrive_b(j):
        wait_on(got_b[j], wb_recv.at[j])
        pl.when(own)(lambda: pass_on(j).start())

    def copy_a(j, dst, sem):
        pl.when(own)(lambda: pltpu.make_async_copy(mine[j], dst, sem).start())
        pl.when(not_own)(lambda: pltpu.make_async_copy(got_a[j], dst, sem).start())

    def copy_b(j, dst, sem):
        pltpu.make_async_copy(got_b[j], dst, sem).start()

    tiles_n = 4 + 2 * chunks

    def load_tile(p, first=None):
        p = p % tiles_n
        slot = p % 4
        if p < 4:
            left = ring.at[slot, :, pl.ds(0, half_w)] if p < 3 else ring.at[slot, pl.ds(0, half_w), :]
            right = ring.at[slot, :, pl.ds(half_w, half_w)] if p < 3 else ring.at[slot, pl.ds(half_w, half_w), :]
            if first is not None:
                @pl.when(first)
                def _():
                    arrive_a(p)
                    arrive_b(p)
            copy_a(p, left, ring_sem.at[slot, 0])
            copy_b(p, right, ring_sem.at[slot, 1])
        else:
            m, is_down = (p - 4) // 2, (p - 4) % 2
            j = 4 + 2 * (m % parts) + is_down
            arrive, copy = (arrive_a, copy_a) if m < parts else (arrive_b, copy_b)
            if first is not None:
                pl.when(first)(lambda: arrive(j))
            copy(j, ring.at[slot], ring_sem.at[slot, 0])

    def wait_tile(slot, halves=None):
        if halves is None:
            wait_on(ring.at[slot], ring_sem.at[slot, 0])
        elif halves == 'cols':
            for k in range(2):
                wait_on(ring.at[slot, :, pl.ds(k * half_w, half_w)], ring_sem.at[slot, k])
        else:
            for k in range(2):
                wait_on(ring.at[slot, pl.ds(k * half_w, half_w), :], ring_sem.at[slot, k])

    def load_x(i, slot):
        seq = 2 * i + core
        dst, sem = x_buf.at[slot], x_sem.at[slot]

        @pl.when(stage == 0)
        def _():
            pltpu.make_async_copy(x_hbm.at[seq], dst, sem).start()

        @pl.when(stage > 0)
        def _():
            wait_on(inbox.at[i], in_recv.at[i])

            @pl.when(is_odd & not_own)
            def _():
                pltpu.make_async_copy(hidden.at[seq], dst, sem).start()

            @pl.when(is_even | own)
            def _():
                pltpu.make_async_copy(inbox.at[i], dst, sem).start()

            @pl.when(is_odd & own)
            def _():
                @pl.when(i >= 2)
                def _():
                    remote(inbox.at[i], hidden.at[seq], f_send.at[slot], st_recv.at[0, i], partner).wait_send()
                remote(inbox.at[i], hidden.at[seq], f_send.at[slot], st_recv.at[0, i], partner).start()

    def sends(i, src):
        seq, slot = 2 * i + core, lax.rem(i, 2)
        return [
            (is_even & own, remote(src, hidden.at[seq], y_send.at[slot], in_recv.at[i], y_peer)),
            (is_even & not_own, remote(src, inbox.at[i], y_send.at[slot], in_recv.at[i], y_peer)),
            (is_odd, remote(src, hidden.at[seq], y_send.at[slot], st_recv.at[core, i], y_store)),
            (stage == 1, remote(src, inbox.at[i], x_send.at[slot], in_recv.at[i], x_peer)),
            (not_own, remote(src, hidden.at[seq], c_send.at[slot], st_recv.at[0, i], partner)),
        ]

    def each_send(i, what):
        @pl.when(own)
        def _():
            for cond, copy in sends(i, hidden.at[2 * i + core]):
                pl.when(cond)(functools.partial(what, copy))

        @pl.when(not_own)
        def _():
            for cond, copy in sends(i, ostage.at[i]):
                pl.when(cond)(functools.partial(what, copy))

    def start_sends(i):
        wait_on(out_buf, l_sem)

        @pl.when(i >= 2)
        def _():
            each_send(i - 2, lambda copy: copy.wait_send())
        each_send(i, lambda copy: copy.start())

    def wide(row):
        return jnp.concatenate([small[0, row:row + 1, :], small[0, row + 1:row + 2, :]], axis=-1)

    lane_tile = 128
    group_w = 384
    group_heads = group_w // head_dim
    groups_loc = heads_loc // group_heads
    spans = []
    for r in range(group_heads):
        low, high = r * head_dim, (r + 1) * head_dim
        start, stop = low // lane_tile * lane_tile, -(-high // lane_tile) * lane_tile
        spans.append((start, stop - start, low - start, high - start))
    q_rows = seq_n // 2
    sub = 16
    score_scale = head_dim ** -0.5 * LOG2E

    def attention_group(g, carry):
        base = g * group_w
        rank = jnp.where(g < groups_loc, y, 1 - y)
        head = rank * heads_loc + lax.rem(g, groups_loc) * group_heads
        for qb in range(2):
            q_ds = pl.ds(qb * q_rows, q_rows)
            keys = (qb + 1) * q_rows
            outs = []
            for r, (start, span, low, high) in enumerate(spans):
                col = pl.ds(pl.multiple_of(base + start, lane_tile), span)
                lane = lax.broadcasted_iota(jnp.int32, (keys, span), 1)
                k_val = qkv_buf[1, pl.ds(0, keys), col]
                k_val = jnp.where((lane >= low) & (lane < high), k_val, jnp.zeros_like(k_val))
                q_val = qkv_buf[0, q_ds, col]
                score_buf[r, :, pl.ds(0, keys)] = lax.dot_general(q_val, k_val, (((1,), (1,)), ((), ())), preferred_element_type=F32)
            for r, (start, span, low, high) in enumerate(spans):
                col = pl.ds(pl.multiple_of(base + start, lane_tile), span)
                slope = slopes[head + r]
                for blk in range(q_rows // sub):
                    rows = pl.ds(blk * sub, sub)
                    at = qb * q_rows + blk * sub
                    need = -(-(at + sub) // lane_tile) * lane_tile
                    score = score_buf[r, rows, pl.ds(0, need)] * score_scale + slope * bias[pl.ds(at, sub), pl.ds(0, need)]
                    top = jnp.max(score, axis=-1, keepdims=True)
                    prob = jnp.exp2(score - top)
                    inv = 1.0 / jnp.sum(prob, axis=-1, keepdims=True)
                    prob_buf[r, rows, pl.ds(0, need)] = (prob * inv).astype(BF16)
                    if need < keys:
                        prob_buf[r, rows, pl.ds(need, keys - need)] = jnp.zeros((sub, keys - need), BF16)
                outs.append(jnp.dot(prob_buf[r, :, pl.ds(0, keys)], qkv_buf[2, pl.ds(0, keys), col], preferred_element_type=F32))
            lane = lax.broadcasted_iota(jnp.int32, (q_rows, lane_tile), 1)
            for tile in range(group_w // lane_tile):
                value = None
                for r, (start, span, low, high) in enumerate(spans):
                    at = tile * lane_tile - start
                    if at < 0 or at >= span:
                        continue
                    piece = outs[r][:, at:at + lane_tile]
                    value = piece if value is None else jnp.where(lane >= low - at, piece, value)
                ctx_buf[q_ds, pl.ds(pl.multiple_of(base + tile * lane_tile, lane_tile), lane_tile)] = value.astype(BF16)
        return carry

    at_start = stage == 0

    @pl.when(stage > 0)
    def _():
        for j in range(pieces_n):
            arrive_a(j)
        for j in range(pieces_n):
            arrive_b(j)

    load_x(0, 0)
    for p in range(4):
        load_tile(p, at_start)

    @pl.when(own)
    def _():
        small_local.wait()
        wait_on(small.at[1], small_sem.at[3])
        small_pass.start()

    @pl.when(not_own)
    def _():
        wait_on(small.at[0], small_sem.at[2])
        wait_on(small.at[1], small_sem.at[3])

    def one_unit(i, carry):
        slot = lax.rem(i, 2)
        first = at_start & (i == 0)
        more = i + 1 < units
        wait_on(x_buf.at[slot], x_sem.at[slot])
        length = lens[2 * i + core]

        def bias_block(blk, carry):
            block = 64
            rows = pl.multiple_of(blk * block, block)
            query_pos = rows + lax.broadcasted_iota(jnp.int32, (block, seq_n), 0)
            key_pos = lax.broadcasted_iota(jnp.int32, (block, seq_n), 1)
            allowed = (key_pos <= query_pos) & (key_pos < length)
            bias[pl.ds(rows, block), :] = jnp.where(allowed, (key_pos - query_pos).astype(F32), MASKED)
            return carry

        lax.fori_loop(0, seq_n // 64, bias_block, 0)
        gain1, shift1 = wide(LN1_G), wide(LN1_S)

        def first_norm(rows):
            a_buf[rows, :] = normalize(x_buf[slot, rows, :].astype(F32), gain1, shift1)

        row_blocks(seq_n, first_norm)

        @pl.when(i > 0)
        def _():
            start_sends(i - 1)

        for j in range(3):
            wait_tile(j, 'cols')
            both = jnp.concatenate([small[k, B_QKV + j:B_QKV + j + 1, :] for k in range(2)], axis=-1)
            qkv_buf[j] = (jnp.dot(a_buf[...], ring[j], preferred_element_type=F32) + both).astype(BF16)
            load_tile(j + 4, first)

        lax.fori_loop(0, 2 * groups_loc, attention_group, 0)

        wait_tile(3, 'rows')
        acc[...] = jnp.dot(ctx_buf[...], ring[3], preferred_element_type=F32)
        load_tile(7, first)
        bias_out, bias_down, gain2, shift2 = wide(B_OUT), wide(B_DOWN), wide(LN2_G), wide(LN2_S)

        def second_norm(rows):
            resid = (x_buf[slot, rows, :].astype(F32) + acc[rows, :] + bias_out).astype(BF16).astype(F32)
            acc[rows, :] = resid + bias_down
            a_buf[rows, :] = normalize(resid, gain2, shift2)

        row_blocks(seq_n, second_norm)

        def up(m, into):
            row = B_UP + 2 * lax.rem(m, parts)
            part = m // parts
            both = jnp.concatenate([small[part, pl.ds(row + k, 1), :] for k in range(2)], axis=-1)
            value = jnp.dot(a_buf[...], ring[2 * lax.rem(m, 2)], preferred_element_type=F32) + both
            u_buf[into] = gelu(value).astype(BF16)

        def down(m):
            return jnp.dot(u_buf[lax.rem(m, 2)], ring[2 * lax.rem(m, 2) + 1], preferred_element_type=F32)

        wait_tile(0)
        up(0, 0)
        load_tile(8, first)

        def mlp(m, carry):
            wait_tile(2 * lax.rem(m + 1, 2))
            wait_tile(2 * lax.rem(m, 2) + 1)
            up(m + 1, lax.rem(m + 1, 2))
            acc[...] += down(m)
            for at in range(chunks - 1):
                later = (6 + 2 * at + 4, 5 + 2 * at + 4)

                @pl.when(m == at)
                def _(later=later):
                    for p in later:
                        if p < tiles_n:
                            load_tile(p, first)
                        else:
                            pl.when(more)(functools.partial(load_tile, p))
            return carry

        lax.fori_loop(0, chunks - 1, mlp, 0)

        @pl.when(more)
        def _():
            load_x(i + 1, 1 - slot)

        wait_tile(3)
        out_buf[...] = (acc[...] + down(chunks - 1)).astype(BF16)
        pl.when(more)(functools.partial(load_tile, tiles_n + 3))

        @pl.when(own)
        def _():
            pltpu.make_async_copy(out_buf, hidden.at[2 * i + core], l_sem).start()

        @pl.when(not_own)
        def _():
            pltpu.make_async_copy(out_buf, ostage.at[i], l_sem).start()
        return carry

    lax.fori_loop(0, units, one_unit, 0)
    start_sends(units - 1)

    for i in (units - 2, units - 1):
        each_send(i, lambda copy: copy.wait_send())

        @pl.when(is_odd & own)
        def _(i=i):
            remote(inbox.at[i], hidden.at[2 * i + core], f_send.at[i % 2], st_recv.at[0, i], partner).wait_send()

    for j in range(pieces_n):
        wait_on(mine[j], w_send.at[j])
        pl.when(own)(lambda j=j: pass_on(j).wait_send())
    wait_on(small_hbm, small_sem.at[1])
    pl.when(own)(lambda: small_pass.wait_send())

    def drain(i, carry):
        wait_on(hidden.at[i], st_recv.at[0, i])
        pl.when(is_even & not_own)(lambda: wait_on(hidden.at[i], st_recv.at[1, i]))
        return carry

    lax.fori_loop(0, units, drain, 0)


def solution(mesh):
    in_specs = (P('dp'), P('dp'), P('pp'), P('pp'), P('pp', None, None, 'tp'), P('pp', None, 'tp', None), P('pp', 'tp', None), P('pp'), P('pp'), P('pp'), P('pp', None, 'tp'), P('pp', 'tp'), P('pp', 'tp', None), P('pp'))

    def per_device(x_in, seq_lens, ln1_gain, ln1_shift, w_qkv, b_qkv, w_out, b_out, ln2_gain, ln2_shift, w_up, b_up, w_down, b_down):
        micro_n, batch_n, seq_n, width = x_in.shape
        total = micro_n * batch_n
        units = total // 2
        half_w = w_out.shape[1]
        head_dim = b_qkv.shape[3]
        heads_n = width // head_dim
        up_w = w_up.shape[2]
        parts = up_w // width
        packed = jnp.concatenate([v[0].reshape(-1) for v in (ln1_gain, ln1_shift, b_out, ln2_gain, ln2_shift, b_down, b_qkv, b_up)])
        packed = packed.astype(F32).reshape(-1, half_w)
        packed = jnp.pad(packed, ((0, -packed.shape[0] % 8), (0, 0)))
        slopes = jnp.asarray(np.array(alibi_slopes(heads_n), np.float32) * np.float32(LOG2E))
        wqkv = jnp.transpose(w_qkv[0], (1, 0, 2))
        weights = (wqkv, w_out[0], w_up[0], w_down[0])
        hbm = pl.BlockSpec(memory_space=pl.ANY)
        smem = pl.BlockSpec(memory_space=pltpu.SMEM)
        seq_t = lambda n: jax.ShapeDtypeStruct((n, seq_n, width), BF16)
        half_t = [
            jax.ShapeDtypeStruct(wqkv.shape, BF16),
            jax.ShapeDtypeStruct((half_w, width), BF16),
            jax.ShapeDtypeStruct((parts, width, width), BF16),
            jax.ShapeDtypeStruct((up_w, width), BF16),
        ]
        pieces_n = 4 + 2 * parts
        flops = 2 * units * seq_n * width * (4 * width + 4 * up_w)
        outs = pl.pallas_call(
            functools.partial(stage_kernel, units, head_dim),
            out_shape=[seq_t(total), seq_t(units), seq_t(units)] + half_t + half_t,
            in_specs=[hbm, smem, smem, hbm] + [hbm] * 4,
            out_specs=[hbm] * 11,
            scratch_shapes=[
                pltpu.VMEM((2,) + packed.shape, F32),
                pltpu.VMEM((2, seq_n, width), BF16),
                pltpu.VMEM((seq_n, width), BF16),
                pltpu.VMEM((3, seq_n, width), BF16),
                pltpu.VMEM((seq_n, width), BF16),
                pltpu.VMEM((seq_n, width), F32),
                pltpu.VMEM((2, seq_n, width), BF16),
                pltpu.VMEM((seq_n, seq_n), F32),
                pltpu.VMEM((4, seq_n // 2, seq_n), F32),
                pltpu.VMEM((4, seq_n // 2, seq_n), BF16),
                pltpu.VMEM((seq_n, width), BF16),
                pltpu.VMEM((4, width, width), BF16),
                pltpu.SemaphoreType.DMA((5,)),
                pltpu.SemaphoreType.DMA((pieces_n,)),
                pltpu.SemaphoreType.DMA((pieces_n,)),
                pltpu.SemaphoreType.DMA((pieces_n,)),
                pltpu.SemaphoreType.DMA((pieces_n,)),
                pltpu.SemaphoreType.DMA((units,)),
                pltpu.SemaphoreType.DMA((2, units)),
                pltpu.SemaphoreType.DMA((4, 2)),
                pltpu.SemaphoreType.DMA((2,)),
                pltpu.SemaphoreType.DMA,
                pltpu.SemaphoreType.DMA((2,)),
                pltpu.SemaphoreType.DMA((2,)),
                pltpu.SemaphoreType.DMA((2,)),
                pltpu.SemaphoreType.DMA((2,)),
            ],
            compiler_params=pltpu.CompilerParams(collective_id=0, has_side_effects=True, vmem_limit_bytes=60 * 1024 * 1024),
            cost_estimate=pl.CostEstimate(flops=flops, bytes_accessed=1 << 31, transcendentals=0),
            name='stage_kernel',
        )(x_in.reshape(total, seq_n, width), seq_lens.reshape(total), slopes, packed, *weights)
        return outs[0].reshape((1,) + x_in.shape)

    return jax.shard_map(per_device, mesh=mesh, in_specs=in_specs, out_specs=P('pp', 'dp'), check_vma=False)
```

```python
import functools
import math

import jax
import jax.numpy as jnp
import numpy as np
from jax import lax
from jax.experimental import pallas as pl
from jax.experimental.pallas import tpu as pltpu
from jax.sharding import PartitionSpec as P

MESH = pl.DeviceIdType.MESH
LOG2E = math.log2(math.e)
MASKED = -1e34
F32 = jnp.float32
BF16 = jnp.bfloat16
LN1_G, LN1_S, B_OUT, LN2_G, LN2_S, B_DOWN, B_QKV, B_UP = 0, 2, 4, 6, 8, 10, 12, 15


def alibi_slopes(heads_n):
    closest = 2 ** int(math.floor(math.log2(heads_n)))
    base_rate = 2.0 ** (-8.0 / closest)
    slope_list = [base_rate ** (head_idx + 1) for head_idx in range(closest)]
    extra_rate = 2.0 ** (-4.0 / closest)
    return slope_list + [extra_rate ** (2 * head_idx + 1) for head_idx in range(min(closest, heads_n - closest))]


def normalize(val_f, gain, shift):
    width = val_f.shape[-1]
    mean_val = jnp.sum(val_f, axis=-1, keepdims=True) * (1.0 / width)
    centered = val_f - mean_val
    var_val = jnp.sum(centered * centered, axis=-1, keepdims=True) * (1.0 / width)
    normed = centered * lax.rsqrt(var_val + 1e-5)
    return (normed * gain + shift).astype(BF16)


def row_blocks(rows_n, body, block=16, unroll=8):
    def some(step, carry):
        for k in range(unroll):
            body(pl.multiple_of(step * (block * unroll) + k * block, block), block)
        return carry

    lax.fori_loop(0, rows_n // (block * unroll), some, 0)


def gelu(val):
    inner = val * (0.7978845608028654 + (0.7978845608028654 * 0.044715) * (val * val))
    half = 0.5 * val
    return half + half * jnp.tanh(inner)


def stage_kernel(
    units, head_dim,
    x_hbm, lens, slopes, small_hbm, wqkv, wout, wup, wdown,
    hidden, inbox, ostage, wa_qkv, wa_out, wa_up, wa_down, wb_qkv, wb_out, wb_up, wb_down,
    small, x_buf, a_buf, qkv_buf, ctx_buf, h_buf, acc, u_buf, bias, score_buf, prob_buf, out_buf, ring,
    small_sem, wa_recv, wb_recv, w_send, w_fwd, in_recv, st_recv, ring_sem, x_sem, l_sem,
    y_send, c_send, x_send, f_send,
):
    dp = lax.axis_index('dp')
    y = lax.axis_index('tp')
    pp = lax.axis_index('pp')
    core = lax.rem(pp, 2)
    chip_x = pp // 2
    odd = lax.rem(chip_x + y, 2)
    stage = 2 * chip_x + odd
    own = core == odd
    not_own = core != odd
    is_odd = odd == 1
    is_even = odd == 0
    partner = (dp, y, 2 * chip_x + 1 - core)
    y_peer = (dp, 1 - y, pp)
    y_store = (dp, 1 - y, 2 * chip_x + 1)
    y_other = (dp, 1 - y, 2 * chip_x + 1 - core)
    x_peer = (dp, y, lax.rem(pp + 2, 4))
    seq_n, width = a_buf.shape
    half_w = wout.shape[0]
    heads_loc = half_w // head_dim
    parts = wup.shape[1] // width
    chunks = 2 * parts

    barrier = pltpu.get_barrier_semaphore()
    for other in (partner, y_peer, y_other, x_peer):
        pl.semaphore_signal(barrier, inc=1, device_id=other, device_id_type=MESH)
    pl.semaphore_wait(barrier, 4)

    def remote(src, dst, send_sem, recv_sem, device):
        return pltpu.make_async_remote_copy(src_ref=src, dst_ref=dst, send_sem=send_sem, recv_sem=recv_sem, device_id=device, device_id_type=MESH)

    def wait_on(ref, sem):
        pltpu.make_async_copy(ref, ref, sem).wait()

    def pieces(qkv, out, up, down, up_cut):
        found = [qkv.at[j] for j in range(3)] + [out]
        for m in range(parts):
            found.append(up.at[:, pl.ds(m * width, width)] if up_cut else up.at[m])
            found.append(down.at[pl.ds(m * width, width), :])
        return found

    mine = pieces(wqkv, wout, wup, wdown, True)
    got_a = pieces(wa_qkv, wa_out, wa_up, wa_down, False)
    got_b = pieces(wb_qkv, wb_out, wb_up, wb_down, False)
    pieces_n = len(mine)

    small_local = pltpu.make_async_copy(small_hbm, small.at[0], small_sem.at[0])
    small_give = remote(small_hbm, small.at[0], small_sem.at[1], small_sem.at[2], partner)
    small_cross = remote(small_hbm, small.at[1], small_sem.at[1], small_sem.at[3], y_peer)
    small_pass = remote(small.at[1], small.at[1], small_sem.at[4], small_sem.at[3], partner)

    @pl.when(own)
    def _():
        small_local.start()
        small_give.start()
        for j in range(pieces_n):
            remote(mine[j], got_a[j], w_send.at[j], wa_recv.at[j], partner).start()

    @pl.when(not_own)
    def _():
        small_cross.start()
        for j in range(pieces_n):
            remote(mine[j], got_b[j], w_send.at[j], wb_recv.at[j], y_peer).start()

    def pass_on(j):
        return remote(got_b[j], got_b[j], w_fwd.at[j], wb_recv.at[j], partner)

    def arrive_a(j):
        pl.when(not_own)(lambda: wait_on(got_a[j], wa_recv.at[j]))

    def arrive_b(j):
        wait_on(got_b[j], wb_recv.at[j])
        pl.when(own)(lambda: pass_on(j).start())

    def copy_a(j, dst, sem):
        pl.when(own)(lambda: pltpu.make_async_copy(mine[j], dst, sem).start())
        pl.when(not_own)(lambda: pltpu.make_async_copy(got_a[j], dst, sem).start())

    def copy_b(j, dst, sem):
        pltpu.make_async_copy(got_b[j], dst, sem).start()

    tiles_n = 4 + 2 * chunks

    def load_tile(p, first=None):
        p = p % tiles_n
        slot = p % 4
        if p < 4:
            left = ring.at[slot, :, pl.ds(0, half_w)] if p < 3 else ring.at[slot, pl.ds(0, half_w), :]
            right = ring.at[slot, :, pl.ds(half_w, half_w)] if p < 3 else ring.at[slot, pl.ds(half_w, half_w), :]
            if first is not None:
                @pl.when(first)
                def _():
                    arrive_a(p)
                    arrive_b(p)
            copy_a(p, left, ring_sem.at[slot, 0])
            copy_b(p, right, ring_sem.at[slot, 1])
        else:
            m, is_down = (p - 4) // 2, (p - 4) % 2
            j = 4 + 2 * (m % parts) + is_down
            arrive, copy = (arrive_a, copy_a) if m < parts else (arrive_b, copy_b)
            if first is not None:
                pl.when(first)(lambda: arrive(j))
            copy(j, ring.at[slot], ring_sem.at[slot, 0])

    def wait_tile(slot, halves=None):
        if halves is None:
            wait_on(ring.at[slot], ring_sem.at[slot, 0])
        elif halves == 'cols':
            for k in range(2):
                wait_on(ring.at[slot, :, pl.ds(k * half_w, half_w)], ring_sem.at[slot, k])
        else:
            for k in range(2):
                wait_on(ring.at[slot, pl.ds(k * half_w, half_w), :], ring_sem.at[slot, k])

    half_n = seq_n // 2

    def half_of(ref, seq, h):
        return ref.at[seq, pl.ds(pl.multiple_of(h * half_n, half_n), half_n), :]

    def load_x(i, h):
        seq, slot = 2 * i + core, lax.rem(i, 2)
        dst, sem = half_of(x_buf, slot, h), x_sem.at[slot, h]

        @pl.when(stage == 0)
        def _():
            pltpu.make_async_copy(half_of(x_hbm, seq, h), dst, sem).start()

        @pl.when(stage > 0)
        def _():
            wait_on(half_of(inbox, i, h), in_recv.at[i, h])

            @pl.when(is_odd & not_own)
            def _():
                pltpu.make_async_copy(half_of(hidden, seq, h), dst, sem).start()

            @pl.when(is_even | own)
            def _():
                pltpu.make_async_copy(half_of(inbox, i, h), dst, sem).start()

            @pl.when(is_odd & own)
            def _():
                passed = remote(half_of(inbox, i, h), half_of(hidden, seq, h), f_send.at[slot, h], st_recv.at[0, i, h], partner)
                pl.when(i >= 2)(lambda: passed.wait_send())
                passed.start()

    def sends(i, h, src):
        seq, slot = 2 * i + core, lax.rem(i, 2)
        kept, taken = half_of(hidden, seq, h), half_of(inbox, i, h)
        return [
            (is_even & own, remote(src, kept, y_send.at[slot, h], in_recv.at[i, h], y_peer)),
            (is_even & not_own, remote(src, taken, y_send.at[slot, h], in_recv.at[i, h], y_peer)),
            (is_odd, remote(src, kept, y_send.at[slot, h], st_recv.at[core, i, h], y_store)),
            (stage == 1, remote(src, taken, x_send.at[slot, h], in_recv.at[i, h], x_peer)),
            (not_own, remote(src, kept, c_send.at[slot, h], st_recv.at[0, i, h], partner)),
        ]

    def each_send(i, h, what):
        @pl.when(own)
        def _():
            for cond, copy in sends(i, h, half_of(hidden, 2 * i + core, h)):
                pl.when(cond)(functools.partial(what, copy))

        @pl.when(not_own)
        def _():
            for cond, copy in sends(i, h, half_of(ostage, i, h)):
                pl.when(cond)(functools.partial(what, copy))

    def store_out(i, h):
        rows = pl.ds(pl.multiple_of(h * half_n, half_n), half_n)

        @pl.when(own)
        def _():
            pltpu.make_async_copy(out_buf.at[rows, :], half_of(hidden, 2 * i + core, h), l_sem.at[h]).start()

        @pl.when(not_own)
        def _():
            pltpu.make_async_copy(out_buf.at[rows, :], half_of(ostage, i, h), l_sem.at[h]).start()

    def start_sends(i, h):
        wait_on(out_buf.at[pl.ds(pl.multiple_of(h * half_n, half_n), half_n), :], l_sem.at[h])
        pl.when(i >= 2)(lambda: each_send(i - 2, h, lambda copy: copy.wait_send()))
        each_send(i, h, lambda copy: copy.start())

    passes = units + 2

    def plan(p):
        head, tail = p < 2, p >= units
        i = jnp.where(head, 0, jnp.where(tail, units - 1, p - 1))
        low = jnp.where(head, p, jnp.where(tail, p - units, 0))
        whole = jnp.logical_not(head | tail)
        return i, low, jnp.where(whole, 2, low + 1), whole

    def over_halves(p, what):
        i, low, high, _ = plan(p)

        def one(h, carry):
            what(i, h)
            return carry

        lax.fori_loop(low, high, one, 0)

    def wide(row):
        return jnp.concatenate([small[0, row:row + 1, :], small[0, row + 1:row + 2, :]], axis=-1)

    lane_tile = 128
    group_w = 384
    group_heads = group_w // head_dim
    groups_loc = heads_loc // group_heads
    spans = []
    for r in range(group_heads):
        low, high = r * head_dim, (r + 1) * head_dim
        start, stop = low // lane_tile * lane_tile, -(-high // lane_tile) * lane_tile
        spans.append((start, stop - start, low - start, high - start))
    q_rows = seq_n // 2
    sub = 16
    score_scale = head_dim ** -0.5 * LOG2E

    def attention_group(g, blocks):
        static = isinstance(g, int)
        base = g * group_w
        rank = (y if g < groups_loc else 1 - y) if static else jnp.where(g < groups_loc, y, 1 - y)
        head = rank * heads_loc + (g % groups_loc if static else lax.rem(g, groups_loc)) * group_heads

        def columns(start, size):
            return pl.ds(base + start if static else pl.multiple_of(base + start, lane_tile), size)

        for q_low, pos, keys, skips in blocks:
            q_ds = pl.ds(q_low, q_rows)
            outs = []
            for r, (start, span, low, high) in enumerate(spans):
                col = columns(start, span)
                lane = lax.broadcasted_iota(jnp.int32, (keys, span), 1)
                k_val = qkv_buf[1, pl.ds(0, keys), col]
                k_val = jnp.where((lane >= low) & (lane < high), k_val, jnp.zeros_like(k_val))
                q_val = qkv_buf[0, q_ds, col]
                score_buf[r, :, pl.ds(0, keys)] = lax.dot_general(q_val, k_val, (((1,), (1,)), ((), ())), preferred_element_type=F32)
            for r, (start, span, low, high) in enumerate(spans):
                slope = slopes[head + r]
                for blk in range(q_rows // sub):
                    rows = pl.ds(blk * sub, sub)
                    need = keys
                    at = pl.ds(pos + blk * sub, sub) if skips else pl.ds(pl.multiple_of(pos + blk * sub, sub), sub)
                    if skips:
                        need = -(-(pos + (blk + 1) * sub) // lane_tile) * lane_tile
                    score = score_buf[r, rows, pl.ds(0, need)] * score_scale + slope * bias[at, pl.ds(0, need)]
                    top = jnp.max(score, axis=-1, keepdims=True)
                    prob = jnp.exp2(score - top)
                    inv = 1.0 / jnp.sum(prob, axis=-1, keepdims=True)
                    prob_buf[r, rows, pl.ds(0, need)] = (prob * inv).astype(BF16)
                    if need < keys:
                        prob_buf[r, rows, pl.ds(need, keys - need)] = jnp.zeros((sub, keys - need), BF16)
                outs.append(jnp.dot(prob_buf[r, :, pl.ds(0, keys)], qkv_buf[2, pl.ds(0, keys), columns(start, span)], preferred_element_type=F32))
            lane = lax.broadcasted_iota(jnp.int32, (q_rows, lane_tile), 1)
            for tile in range(group_w // lane_tile):
                value = None
                for r, (start, span, low, high) in enumerate(spans):
                    at = tile * lane_tile - start
                    if at < 0 or at >= span:
                        continue
                    piece = outs[r][:, at:at + lane_tile]
                    value = piece if value is None else jnp.where(lane >= low - at, piece, value)
                ctx_buf[q_ds, columns(tile * lane_tile, lane_tile)] = value.astype(BF16)

    at_start = stage == 0

    @pl.when(stage > 0)
    def _():
        for j in range(pieces_n):
            arrive_a(j)
        for j in range(pieces_n):
            arrive_b(j)

    load_x(0, 0)
    for p in range(4):
        load_tile(p, at_start)

    @pl.when(own)
    def _():
        small_local.wait()
        wait_on(small.at[1], small_sem.at[3])
        small_pass.start()

    @pl.when(not_own)
    def _():
        wait_on(small.at[0], small_sem.at[2])
        wait_on(small.at[1], small_sem.at[3])

    for j in (1, 2):
        qkv_buf[j, pl.ds(half_n, half_n), :] = jnp.zeros((half_n, width), BF16)

    def work(p, i, h, first, more):
        whole = h is None
        rows_n = seq_n if whole else half_n
        low = 0 if whole else pl.multiple_of(h * half_n, half_n)
        slot = lax.rem(i, 2)
        here = pl.ds(0, rows_n)
        kv_rows = pl.ds(low, rows_n)
        for k in range(2) if whole else (h,):
            wait_on(half_of(x_buf, slot, k), x_sem.at[slot, k])
        length = lens[2 * i + core]

        def bias_block(blk, carry):
            block = 64
            rows = pl.multiple_of(low + blk * block, block)
            query_pos = rows + lax.broadcasted_iota(jnp.int32, (block, seq_n), 0)
            key_pos = lax.broadcasted_iota(jnp.int32, (block, seq_n), 1)
            allowed = (key_pos <= query_pos) & (key_pos < length)
            bias[pl.ds(rows, block), :] = jnp.where(allowed, (key_pos - query_pos).astype(F32), MASKED)
            return carry

        lax.fori_loop(0, rows_n // 64, bias_block, 0)
        gain1, shift1 = wide(LN1_G), wide(LN1_S)

        def first_norm(at, size):
            a_buf[pl.ds(at, size), :] = normalize(x_buf[slot, pl.ds(low + at, size), :].astype(F32), gain1, shift1)

        row_blocks(rows_n, first_norm)
        pl.when(p > 0)(lambda: over_halves(p - 1, start_sends))

        def project(j, start, size):
            both = jnp.concatenate([small[k, B_QKV + j:B_QKV + j + 1, :] for k in range(2)], axis=-1)
            value = jnp.dot(a_buf[here, :], ring[j, :, pl.ds(start, size)], preferred_element_type=F32)
            qkv_buf[j, here if j == 0 else kv_rows, pl.ds(start, size)] = (value + both[:, start:start + size]).astype(BF16)

        def out_part(start, size):
            part = pl.ds(start, size)
            return jnp.dot(ctx_buf[here, part], ring[3, part, :], preferred_element_type=F32)

        if whole:
            cut = 2 * width // 3
            blocks = [(qb * q_rows, qb * q_rows, (qb + 1) * q_rows, True) for qb in range(2)]
            for j in range(3):
                wait_tile(j, 'cols')
                project(j, 0, cut)
            wait_tile(3, 'rows')
            project(0, cut, width - cut)
            attention_group(0, blocks)
            project(1, cut, width - cut)
            attention_group(1, blocks)
            project(2, cut, width - cut)
            for j in range(3):
                load_tile(j + 4, first)
            attention_group(2, blocks)
            acc[...] = out_part(0, half_w)
            attention_group(3, blocks)
            attended = acc[...] + out_part(half_w, half_w)
        else:
            for j in range(3):
                wait_tile(j, 'cols')
                project(j, 0, width)
                load_tile(j + 4, first)
            blocks = [(0, low, seq_n, False)]

            def some_heads(g, carry):
                attention_group(g, blocks)
                return carry

            lax.fori_loop(0, 2 * groups_loc, some_heads, 0)
            wait_tile(3, 'rows')
            attended = out_part(0, width)
        bias_out, bias_down, gain2, shift2 = wide(B_OUT), wide(B_DOWN), wide(LN2_G), wide(LN2_S)
        resid = (x_buf[slot, kv_rows, :].astype(F32) + attended + bias_out).astype(BF16)
        h_buf[here, :] = resid
        acc[here, :] = resid.astype(F32) + bias_down
        load_tile(7, first)

        def second_norm(at, size):
            rows = pl.ds(at, size)
            a_buf[rows, :] = normalize(h_buf[rows, :].astype(F32), gain2, shift2)

        row_blocks(rows_n, second_norm)

        def up(m, into):
            row = B_UP + 2 * lax.rem(m, parts)
            part = m // parts
            both = jnp.concatenate([small[part, pl.ds(row + k, 1), :] for k in range(2)], axis=-1)
            value = jnp.dot(a_buf[here, :], ring[2 * lax.rem(m, 2)], preferred_element_type=F32) + both
            u_buf[into, here, :] = gelu(value).astype(BF16)

        def down(m):
            return jnp.dot(u_buf[lax.rem(m, 2), here, :], ring[2 * lax.rem(m, 2) + 1], preferred_element_type=F32)

        wait_tile(0)
        up(0, 0)
        load_tile(8, first)

        def mlp(m, carry):
            wait_tile(2 * lax.rem(m + 1, 2))
            wait_tile(2 * lax.rem(m, 2) + 1)
            up(m + 1, lax.rem(m + 1, 2))
            acc[here, :] += down(m)
            for at in range(chunks - 1):
                later = (6 + 2 * at + 4, 5 + 2 * at + 4)

                @pl.when(m == at)
                def _(later=later):
                    for t in later:
                        if t < tiles_n:
                            load_tile(t, first)
                        else:
                            pl.when(more)(functools.partial(load_tile, t))
            return carry

        lax.fori_loop(0, chunks - 1, mlp, 0)
        pl.when(more)(lambda: over_halves(p + 1, load_x))
        wait_tile(3)
        out_buf[kv_rows, :] = (acc[here, :] + down(chunks - 1)).astype(BF16)
        pl.when(more)(functools.partial(load_tile, tiles_n + 3))
        over_halves(p, store_out)

    def one_pass(p, carry):
        i, h, _, whole = plan(p)
        first = at_start & (p == 0)
        more = p + 1 < passes
        pl.when(whole)(lambda: work(p, i, None, first, more))
        pl.when(jnp.logical_not(whole))(lambda: work(p, i, h, first, more))
        return carry

    lax.fori_loop(0, passes, one_pass, 0)
    over_halves(passes - 1, start_sends)

    def settle(n, carry):
        i, h = units - 2 + n // 2, lax.rem(n, 2)
        each_send(i, h, lambda copy: copy.wait_send())

        @pl.when(is_odd & own)
        def _():
            remote(half_of(inbox, i, h), half_of(hidden, 2 * i + core, h), f_send.at[lax.rem(i, 2), h], st_recv.at[0, i, h], partner).wait_send()
        return carry

    lax.fori_loop(0, 4, settle, 0)

    for j in range(pieces_n):
        wait_on(mine[j], w_send.at[j])
        pl.when(own)(lambda j=j: pass_on(j).wait_send())
    wait_on(small_hbm, small_sem.at[1])
    pl.when(own)(lambda: small_pass.wait_send())

    def drain(n, carry):
        i, h = n // 2, lax.rem(n, 2)
        wait_on(half_of(hidden, i, h), st_recv.at[0, i, h])
        pl.when(is_even & not_own)(lambda: wait_on(half_of(hidden, i, h), st_recv.at[1, i, h]))
        return carry

    lax.fori_loop(0, 2 * units, drain, 0)


def solution(mesh):
    in_specs = (P('dp'), P('dp'), P('pp'), P('pp'), P('pp', None, None, 'tp'), P('pp', None, 'tp', None), P('pp', 'tp', None), P('pp'), P('pp'), P('pp'), P('pp', None, 'tp'), P('pp', 'tp'), P('pp', 'tp', None), P('pp'))

    def per_device(x_in, seq_lens, ln1_gain, ln1_shift, w_qkv, b_qkv, w_out, b_out, ln2_gain, ln2_shift, w_up, b_up, w_down, b_down):
        micro_n, batch_n, seq_n, width = x_in.shape
        total = micro_n * batch_n
        units = total // 2
        half_w = w_out.shape[1]
        head_dim = b_qkv.shape[3]
        heads_n = width // head_dim
        up_w = w_up.shape[2]
        parts = up_w // width
        packed = jnp.concatenate([v[0].reshape(-1) for v in (ln1_gain, ln1_shift, b_out, ln2_gain, ln2_shift, b_down, b_qkv, b_up)])
        packed = packed.astype(F32).reshape(-1, half_w)
        packed = jnp.pad(packed, ((0, -packed.shape[0] % 8), (0, 0)))
        slopes = jnp.asarray(np.array(alibi_slopes(heads_n), np.float32) * np.float32(LOG2E))
        wqkv = jnp.transpose(w_qkv[0], (1, 0, 2))
        weights = (wqkv, w_out[0], w_up[0], w_down[0])
        hbm = pl.BlockSpec(memory_space=pl.ANY)
        smem = pl.BlockSpec(memory_space=pltpu.SMEM)
        seq_t = lambda n: jax.ShapeDtypeStruct((n, seq_n, width), BF16)
        half_t = [
            jax.ShapeDtypeStruct(wqkv.shape, BF16),
            jax.ShapeDtypeStruct((half_w, width), BF16),
            jax.ShapeDtypeStruct((parts, width, width), BF16),
            jax.ShapeDtypeStruct((up_w, width), BF16),
        ]
        pieces_n = 4 + 2 * parts
        flops = 2 * units * seq_n * width * (4 * width + 4 * up_w)
        outs = pl.pallas_call(
            functools.partial(stage_kernel, units, head_dim),
            out_shape=[seq_t(total), seq_t(units), seq_t(units)] + half_t + half_t,
            in_specs=[hbm, smem, smem, hbm] + [hbm] * 4,
            out_specs=[hbm] * 11,
            scratch_shapes=[
                pltpu.VMEM((2,) + packed.shape, F32),
                pltpu.VMEM((2, seq_n, width), BF16),
                pltpu.VMEM((seq_n, width), BF16),
                pltpu.VMEM((3, seq_n, width), BF16),
                pltpu.VMEM((seq_n, width), BF16),
                pltpu.VMEM((seq_n, width), BF16),
                pltpu.VMEM((seq_n, width), F32),
                pltpu.VMEM((2, seq_n, width), BF16),
                pltpu.VMEM((seq_n, seq_n), F32),
                pltpu.VMEM((4, seq_n // 2, seq_n), F32),
                pltpu.VMEM((4, seq_n // 2, seq_n), BF16),
                pltpu.VMEM((seq_n, width), BF16),
                pltpu.VMEM((4, width, width), BF16),
                pltpu.SemaphoreType.DMA((5,)),
                pltpu.SemaphoreType.DMA((pieces_n,)),
                pltpu.SemaphoreType.DMA((pieces_n,)),
                pltpu.SemaphoreType.DMA((pieces_n,)),
                pltpu.SemaphoreType.DMA((pieces_n,)),
                pltpu.SemaphoreType.DMA((units, 2)),
                pltpu.SemaphoreType.DMA((2, units, 2)),
                pltpu.SemaphoreType.DMA((4, 2)),
                pltpu.SemaphoreType.DMA((2, 2)),
                pltpu.SemaphoreType.DMA((2,)),
                pltpu.SemaphoreType.DMA((2, 2)),
                pltpu.SemaphoreType.DMA((2, 2)),
                pltpu.SemaphoreType.DMA((2, 2)),
                pltpu.SemaphoreType.DMA((2, 2)),
            ],
            compiler_params=pltpu.CompilerParams(collective_id=0, has_side_effects=True, vmem_limit_bytes=60 * 1024 * 1024),
            cost_estimate=pl.CostEstimate(flops=flops, bytes_accessed=1 << 31, transcendentals=0),
            name='stage_kernel',
        )(x_in.reshape(total, seq_n, width), seq_lens.reshape(total), slopes, packed, *weights)
        return outs[0].reshape((1,) + x_in.shape)

    return jax.shard_map(per_device, mesh=mesh, in_specs=in_specs, out_specs=P('pp', 'dp'), check_vma=False)
```

```python
import functools
import math

import jax
import jax.numpy as jnp
import numpy as np
from jax import lax
from jax.experimental import pallas as pl
from jax.experimental.pallas import tpu as pltpu
from jax.sharding import PartitionSpec as P

MESH = pl.DeviceIdType.MESH
LOG2E = math.log2(math.e)
MASKED = -1e34
F32 = jnp.float32
BF16 = jnp.bfloat16
LN1_G, LN1_S, B_OUT, LN2_G, LN2_S, B_DOWN, B_QKV, B_UP = 0, 2, 4, 6, 8, 10, 12, 15


def alibi_slopes(heads_n):
    closest = 2 ** int(math.floor(math.log2(heads_n)))
    base_rate = 2.0 ** (-8.0 / closest)
    slope_list = [base_rate ** (head_idx + 1) for head_idx in range(closest)]
    extra_rate = 2.0 ** (-4.0 / closest)
    return slope_list + [extra_rate ** (2 * head_idx + 1) for head_idx in range(min(closest, heads_n - closest))]


def normalize(val_f, gain, shift):
    width = val_f.shape[-1]
    mean_val = jnp.sum(val_f, axis=-1, keepdims=True) * (1.0 / width)
    centered = val_f - mean_val
    var_val = jnp.sum(centered * centered, axis=-1, keepdims=True) * (1.0 / width)
    normed = centered * lax.rsqrt(var_val + 1e-5)
    return (normed * gain + shift).astype(BF16)


def gelu(val):
    inner = val * (0.7978845608028654 + (0.7978845608028654 * 0.044715) * (val * val))
    half = 0.5 * val
    return half + half * jnp.tanh(inner)


def stage_kernel(
    units, head_dim,
    x_hbm, lens, slopes, small_hbm, wqkv, wout, wup, wdown,
    hidden, inbox, ostage, wa_qkv, wa_out, wa_up, wa_down, wb_qkv, wb_out, wb_up, wb_down,
    small, x_buf, a_buf, qkv_buf, ctx_buf, h_buf, acc, u_buf, bias, score_buf, prob_buf, out_buf, ring,
    small_sem, wa_recv, wb_recv, w_send, w_fwd, in_recv, st_recv, ring_sem, x_sem, l_sem,
    y_send, c_send, x_send, f_send,
):
    dp = lax.axis_index('dp')
    y = lax.axis_index('tp')
    pp = lax.axis_index('pp')
    core = lax.rem(pp, 2)
    chip_x = pp // 2
    odd = lax.rem(chip_x + y, 2)
    stage = 2 * chip_x + odd
    own = core == odd
    not_own = core != odd
    is_odd = odd == 1
    is_even = odd == 0
    partner = (dp, y, 2 * chip_x + 1 - core)
    y_peer = (dp, 1 - y, pp)
    y_store = (dp, 1 - y, 2 * chip_x + 1)
    y_other = (dp, 1 - y, 2 * chip_x + 1 - core)
    x_peer = (dp, y, lax.rem(pp + 2, 4))
    seq_n, width = a_buf.shape
    half_w = wout.shape[0]
    heads_loc = half_w // head_dim
    parts = wup.shape[1] // width
    chunks = 2 * parts

    barrier = pltpu.get_barrier_semaphore()
    for other in (partner, y_peer, y_other, x_peer):
        pl.semaphore_signal(barrier, inc=1, device_id=other, device_id_type=MESH)
    pl.semaphore_wait(barrier, 4)

    def remote(src, dst, send_sem, recv_sem, device):
        return pltpu.make_async_remote_copy(src_ref=src, dst_ref=dst, send_sem=send_sem, recv_sem=recv_sem, device_id=device, device_id_type=MESH)

    def wait_on(ref, sem):
        pltpu.make_async_copy(ref, ref, sem).wait()

    def pieces(qkv, out, up, down, up_cut):
        found = [qkv.at[j] for j in range(3)] + [out]
        for m in range(parts):
            found.append(up.at[:, pl.ds(m * width, width)] if up_cut else up.at[m])
            found.append(down.at[pl.ds(m * width, width), :])
        return found

    mine = pieces(wqkv, wout, wup, wdown, True)
    got_a = pieces(wa_qkv, wa_out, wa_up, wa_down, False)
    got_b = pieces(wb_qkv, wb_out, wb_up, wb_down, False)
    pieces_n = len(mine)

    small_local = pltpu.make_async_copy(small_hbm, small.at[0], small_sem.at[0])
    small_give = remote(small_hbm, small.at[0], small_sem.at[1], small_sem.at[2], partner)
    small_cross = remote(small_hbm, small.at[1], small_sem.at[1], small_sem.at[3], y_peer)
    small_pass = remote(small.at[1], small.at[1], small_sem.at[4], small_sem.at[3], partner)

    @pl.when(own)
    def _():
        small_local.start()
        small_give.start()
        for j in range(pieces_n):
            remote(mine[j], got_a[j], w_send.at[j], wa_recv.at[j], partner).start()

    @pl.when(not_own)
    def _():
        small_cross.start()
        for j in range(pieces_n):
            remote(mine[j], got_b[j], w_send.at[j], wb_recv.at[j], y_peer).start()

    def pass_on(j):
        return remote(got_b[j], got_b[j], w_fwd.at[j], wb_recv.at[j], partner)

    def arrive_a(j):
        pl.when(not_own)(lambda: wait_on(got_a[j], wa_recv.at[j]))

    def arrive_b(j):
        wait_on(got_b[j], wb_recv.at[j])
        pl.when(own if j < pieces_n - 1 else own & (stage > 0))(lambda: pass_on(j).start())

    def copy_a(j, dst, sem):
        pl.when(own)(lambda: pltpu.make_async_copy(mine[j], dst, sem).start())
        pl.when(not_own)(lambda: pltpu.make_async_copy(got_a[j], dst, sem).start())

    def copy_b(j, dst, sem):
        pltpu.make_async_copy(got_b[j], dst, sem).start()

    tiles_n = 4 + 2 * chunks
    ring_n = ring.shape[0]

    def load_tile(p, first=None):
        p = p % tiles_n
        slot = p % ring_n
        if p < 4:
            left = ring.at[slot, :, pl.ds(0, half_w)] if p < 3 else ring.at[slot, pl.ds(0, half_w), :]
            right = ring.at[slot, :, pl.ds(half_w, half_w)] if p < 3 else ring.at[slot, pl.ds(half_w, half_w), :]
            if first is not None:
                @pl.when(first)
                def _():
                    arrive_a(p)
                    arrive_b(p)
            copy_a(p, left, ring_sem.at[slot, 0])
            copy_b(p, right, ring_sem.at[slot, 1])
        else:
            m, is_down = (p - 4) // 2, (p - 4) % 2
            j = 4 + 2 * (m % parts) + is_down
            arrive, copy = (arrive_a, copy_a) if m < parts else (arrive_b, copy_b)
            if first is not None:
                pl.when(first)(lambda: arrive(j))
            copy(j, ring.at[slot], ring_sem.at[slot, 0])

    def wait_tile(p):
        slot = p % ring_n
        if p < 4:
            for k in range(2):
                cut = pl.ds(k * half_w, half_w)
                wait_on(ring.at[slot, :, cut] if p < 3 else ring.at[slot, cut, :], ring_sem.at[slot, k])
        else:
            wait_on(ring.at[slot], ring_sem.at[slot, 0])

    half_n = seq_n // 2

    def place(p):
        return 2 * p + core, lax.rem(p, 2)

    def passed_on(p):
        seq, slot = place(p)
        return remote(inbox.at[p], hidden.at[seq], f_send.at[slot], st_recv.at[0, p], partner)

    def load_x(p):
        seq, slot = place(p)
        dst, sem = x_buf.at[slot], x_sem.at[slot]

        @pl.when(stage == 0)
        def _():
            pltpu.make_async_copy(x_hbm.at[seq], dst, sem).start()

        @pl.when(stage > 0)
        def _():
            wait_on(inbox.at[p], in_recv.at[p])

            @pl.when(is_odd & not_own)
            def _():
                pltpu.make_async_copy(hidden.at[seq], dst, sem).start()

            @pl.when(is_even | own)
            def _():
                pltpu.make_async_copy(inbox.at[p], dst, sem).start()

            @pl.when(is_odd & own)
            def _():
                pl.when(p >= 2)(lambda: passed_on(p - 2).wait_send())
                passed_on(p).start()

    def sends(p, src):
        seq, slot = place(p)
        return [
            (is_even & own, remote(src, hidden.at[seq], y_send.at[slot], in_recv.at[p], y_peer)),
            (is_even & not_own, remote(src, inbox.at[p], y_send.at[slot], in_recv.at[p], y_peer)),
            (is_odd, remote(src, hidden.at[seq], y_send.at[slot], st_recv.at[core, p], y_store)),
            (stage == 1, remote(src, inbox.at[p], x_send.at[slot], in_recv.at[p], x_peer)),
            (not_own, remote(src, hidden.at[seq], c_send.at[slot], st_recv.at[0, p], partner)),
        ]

    def each_send(p, what):
        @pl.when(own)
        def _():
            for cond, copy in sends(p, hidden.at[2 * p + core]):
                pl.when(cond)(functools.partial(what, copy))

        @pl.when(not_own)
        def _():
            for cond, copy in sends(p, ostage.at[p]):
                pl.when(cond)(functools.partial(what, copy))

    def store_out(p):
        pl.when(own)(lambda: pltpu.make_async_copy(out_buf, hidden.at[2 * p + core], l_sem).start())
        pl.when(not_own)(lambda: pltpu.make_async_copy(out_buf, ostage.at[p], l_sem).start())

    def start_sends(p):
        wait_on(out_buf, l_sem)
        pl.when(p >= 2)(lambda: each_send(p - 2, lambda copy: copy.wait_send()))
        each_send(p, lambda copy: copy.start())

    def wide(row):
        return jnp.concatenate([small[0, row:row + 1, :], small[0, row + 1:row + 2, :]], axis=-1)

    lane_tile = 128
    group_w = 384
    group_heads = group_w // head_dim
    groups_loc = heads_loc // group_heads
    spans = []
    for r in range(group_heads):
        low, high = r * head_dim, (r + 1) * head_dim
        start, stop = low // lane_tile * lane_tile, -(-high // lane_tile) * lane_tile
        spans.append((start, stop - start, low - start, high - start))
    q_rows = seq_n // 2
    sub = 16
    score_scale = head_dim ** -0.5 * LOG2E

    def scores(g):
        for qb in range(2):
            keys = (qb + 1) * q_rows
            for r, (start, span, low, high) in enumerate(spans):
                col = pl.ds(g * group_w + start, span)
                lane = lax.broadcasted_iota(jnp.int32, (keys, span), 1)
                k_val = qkv_buf[1, pl.ds(0, keys), col]
                k_val = jnp.where((lane >= low) & (lane < high), k_val, jnp.zeros_like(k_val))
                q_val = qkv_buf[0, pl.ds(qb * q_rows, q_rows), col]
                score_buf[qb, r, :, pl.ds(0, keys)] = lax.dot_general(q_val, k_val, (((1,), (1,)), ((), ())), preferred_element_type=F32)

    def soften(g):
        head = (y if g < groups_loc else 1 - y) * heads_loc + g % groups_loc * group_heads
        for qb in range(2):
            keys = (qb + 1) * q_rows
            for r in range(group_heads):
                slope = slopes[head + r]
                for blk in range(q_rows // sub):
                    rows = pl.ds(blk * sub, sub)
                    at = qb * q_rows + blk * sub
                    need = -(-(at + sub) // lane_tile) * lane_tile
                    score = score_buf[qb, r, rows, pl.ds(0, need)] * score_scale + slope * bias[pl.ds(at, sub), pl.ds(0, need)]
                    top = jnp.max(score, axis=-1, keepdims=True)
                    prob = jnp.exp2(score - top)
                    inv = 1.0 / jnp.sum(prob, axis=-1, keepdims=True)
                    prob_buf[qb, r, rows, pl.ds(0, need)] = (prob * inv).astype(BF16)
                    if need < keys:
                        prob_buf[qb, r, rows, pl.ds(need, keys - need)] = jnp.zeros((sub, keys - need), BF16)

    def contexts(g):
        lane = lax.broadcasted_iota(jnp.int32, (q_rows, lane_tile), 1)
        for qb in range(2):
            keys = (qb + 1) * q_rows
            outs = []
            for r, (start, span, low, high) in enumerate(spans):
                v_val = qkv_buf[2, pl.ds(0, keys), pl.ds(g * group_w + start, span)]
                outs.append(jnp.dot(prob_buf[qb, r, :, pl.ds(0, keys)], v_val, preferred_element_type=F32))
            for tile in range(group_w // lane_tile):
                value = None
                for r, (start, span, low, high) in enumerate(spans):
                    at = tile * lane_tile - start
                    if at < 0 or at >= span:
                        continue
                    piece = outs[r][:, at:at + lane_tile]
                    value = piece if value is None else jnp.where(lane >= low - at, piece, value)
                ctx_buf[pl.ds(qb * q_rows, q_rows), pl.ds(g * group_w + tile * lane_tile, lane_tile)] = value.astype(BF16)

    at_start = stage == 0

    @pl.when(stage > 0)
    def _():
        for j in range(pieces_n):
            arrive_a(j)
        for j in range(pieces_n):
            arrive_b(j)

    load_x(jnp.int32(0))
    for p in range(ring_n):
        load_tile(p, at_start)

    @pl.when(own)
    def _():
        small_local.wait()
        wait_on(small.at[1], small_sem.at[3])
        small_pass.start()

    @pl.when(not_own)
    def _():
        wait_on(small.at[0], small_sem.at[2])
        wait_on(small.at[1], small_sem.at[3])

    whole = pl.ds(0, seq_n)
    two = [pl.ds(k * half_n, half_n) for k in range(2)]

    def one_unit(p, carry):
        seq, slot = place(p)
        first = at_start & (p == 0)
        more = p + 1 < units
        wait_on(x_buf.at[slot], x_sem.at[slot])
        length = lens[seq]

        def bias_block(blk, carry):
            block = 64
            rows = pl.multiple_of(blk * block, block)
            query_pos = rows + lax.broadcasted_iota(jnp.int32, (block, seq_n), 0)
            key_pos = lax.broadcasted_iota(jnp.int32, (block, seq_n), 1)
            allowed = (key_pos <= query_pos) & (key_pos < length)
            bias[pl.ds(rows, block), :] = jnp.where(allowed, (key_pos - query_pos).astype(F32), MASKED)
            return carry

        lax.fori_loop(0, seq_n // 64, bias_block, 0)
        gain1, shift1 = wide(LN1_G), wide(LN1_S)

        def first_norm(low):
            for at in range(low, low + half_n, 16):
                a_buf[at:at + 16, :] = normalize(x_buf[slot, at:at + 16, :].astype(F32), gain1, shift1)

        def project(j, start, size, rows=whole):
            both = jnp.concatenate([small[k, B_QKV + j:B_QKV + j + 1, :] for k in range(2)], axis=-1)
            value = jnp.dot(a_buf[rows, :], ring[j, :, pl.ds(start, size)], preferred_element_type=F32)
            qkv_buf[j, rows, pl.ds(start, size)] = (value + both[:, start:start + size]).astype(BF16)

        def out_part(k_low, k_size, low, size):
            part = pl.ds(k_low, k_size)
            acc[:, pl.ds(low, size)] = jnp.dot(ctx_buf[:, part], ring[3, part, pl.ds(low, size)], preferred_element_type=F32)

        bias_out, bias_down, gain2, shift2 = wide(B_OUT), wide(B_DOWN), wide(LN2_G), wide(LN2_S)

        def add_attended(rows):
            resid = (x_buf[slot, rows, :].astype(F32) + acc[rows, :] + jnp.dot(ctx_buf[rows, half_w:], ring[3, half_w:, :], preferred_element_type=F32) + bias_out).astype(BF16)
            h_buf[rows, :] = resid
            acc[rows, :] = resid.astype(F32) + bias_down

        def second_norm(low):
            for at in range(low, low + half_n, 16):
                a_buf[at:at + 16, :] = normalize(h_buf[at:at + 16, :].astype(F32), gain2, shift2)

        def up(m, rows=whole):
            row = B_UP + 2 * lax.rem(m, parts)
            part = m // parts
            both = jnp.concatenate([small[part, pl.ds(row + k, 1), :] for k in range(2)], axis=-1)
            value = jnp.dot(a_buf[rows, :], ring[2 * lax.rem(m, 2)], preferred_element_type=F32) + both
            u_buf[lax.rem(m, 2), rows, :] = gelu(value).astype(BF16)

        def down(m):
            return jnp.dot(u_buf[lax.rem(m, 2)], ring[2 * lax.rem(m, 2) + 1], preferred_element_type=F32)

        cut = 2 * width // 3
        first_norm(0)
        pl.when(p > 0)(lambda: start_sends(p - 1))
        pl.when((stage == 0) & own & (p == 1))(lambda: pass_on(pieces_n - 1).start())
        for j in range(3):
            wait_tile(j)
        project(0, 0, cut, two[0])
        first_norm(half_n)
        project(0, 0, cut, two[1])
        project(1, 0, cut)
        project(2, 0, cut)
        scores(0)
        project(0, cut, width - cut)
        soften(0)
        scores(1)
        contexts(0)
        project(1, cut, width - cut)
        soften(1)
        project(2, cut, width - cut)
        contexts(1)
        for t in (4, 5, 6):
            load_tile(t, first)
        for t in (3, 4):
            wait_tile(t)
        scores(2)
        out_part(0, half_w, 0, cut)
        soften(2)
        scores(3)
        contexts(2)
        out_part(0, half_w, cut, width - cut)
        soften(3)
        contexts(3)
        for rows in two:
            add_attended(rows)
        second_norm(0)
        up(0, two[0])
        second_norm(half_n)
        up(0, two[1])
        load_tile(7, first)
        load_tile(8, first)

        def mlp(m, carry):
            up_slot, down_slot = 2 * lax.rem(m + 1, 2), 2 * lax.rem(m, 2) + 1
            wait_on(ring.at[up_slot], ring_sem.at[up_slot, 0])
            wait_on(ring.at[down_slot], ring_sem.at[down_slot, 0])
            up(m + 1)
            acc[...] += down(m)
            for at in range(chunks - 1):
                @pl.when(m == at)
                def _(at=at):
                    for t in (10 + 2 * at, 9 + 2 * at):
                        if t < tiles_n:
                            load_tile(t, first)
                        else:
                            pl.when(more)(functools.partial(load_tile, t))
            return carry

        lax.fori_loop(0, chunks - 1, mlp, 0)
        pl.when(more)(lambda: load_x(p + 1))
        wait_tile(11)
        out_buf[...] = (acc[...] + down(chunks - 1)).astype(BF16)
        pl.when(more)(functools.partial(load_tile, tiles_n + 3))
        store_out(p)
        return carry

    lax.fori_loop(0, units, one_unit, 0)
    start_sends(jnp.int32(units - 1))

    def settle(n, carry):
        p = units - 2 + n
        each_send(p, lambda copy: copy.wait_send())
        pl.when(is_odd & own)(lambda: passed_on(p).wait_send())
        return carry

    lax.fori_loop(0, 2, settle, 0)

    for j in range(pieces_n):
        wait_on(mine[j], w_send.at[j])
        pl.when(own)(lambda j=j: pass_on(j).wait_send())
    wait_on(small_hbm, small_sem.at[1])
    pl.when(own)(lambda: small_pass.wait_send())

    def drain(p, carry):
        wait_on(hidden.at[p], st_recv.at[0, p])
        pl.when(is_even & not_own)(lambda: wait_on(hidden.at[p], st_recv.at[1, p]))
        return carry

    lax.fori_loop(0, units, drain, 0)


def solution(mesh):
    in_specs = (P('dp'), P('dp'), P('pp'), P('pp'), P('pp', None, None, 'tp'), P('pp', None, 'tp', None), P('pp', 'tp', None), P('pp'), P('pp'), P('pp'), P('pp', None, 'tp'), P('pp', 'tp'), P('pp', 'tp', None), P('pp'))

    def per_device(x_in, seq_lens, ln1_gain, ln1_shift, w_qkv, b_qkv, w_out, b_out, ln2_gain, ln2_shift, w_up, b_up, w_down, b_down):
        micro_n, batch_n, seq_n, width = x_in.shape
        total = micro_n * batch_n
        units = total // 2
        half_w = w_out.shape[1]
        head_dim = b_qkv.shape[3]
        heads_n = width // head_dim
        up_w = w_up.shape[2]
        parts = up_w // width
        packed = jnp.concatenate([v[0].reshape(-1) for v in (ln1_gain, ln1_shift, b_out, ln2_gain, ln2_shift, b_down, b_qkv, b_up)])
        packed = packed.astype(F32).reshape(-1, half_w)
        packed = jnp.pad(packed, ((0, -packed.shape[0] % 8), (0, 0)))
        slopes = jnp.asarray(np.array(alibi_slopes(heads_n), np.float32) * np.float32(LOG2E))
        wqkv = jnp.transpose(w_qkv[0], (1, 0, 2))
        weights = (wqkv, w_out[0], w_up[0], w_down[0])
        hbm = pl.BlockSpec(memory_space=pl.ANY)
        smem = pl.BlockSpec(memory_space=pltpu.SMEM)
        seq_t = lambda n: jax.ShapeDtypeStruct((n, seq_n, width), BF16)
        half_t = [
            jax.ShapeDtypeStruct(wqkv.shape, BF16),
            jax.ShapeDtypeStruct((half_w, width), BF16),
            jax.ShapeDtypeStruct((parts, width, width), BF16),
            jax.ShapeDtypeStruct((up_w, width), BF16),
        ]
        pieces_n = 4 + 2 * parts
        flops = 2 * units * seq_n * width * (4 * width + 4 * up_w)
        outs = pl.pallas_call(
            functools.partial(stage_kernel, units, head_dim),
            out_shape=[seq_t(total), seq_t(units), seq_t(units)] + half_t + half_t,
            in_specs=[hbm, smem, smem, hbm] + [hbm] * 4,
            out_specs=[hbm] * 11,
            scratch_shapes=[
                pltpu.VMEM((2,) + packed.shape, F32),
                pltpu.VMEM((2, seq_n, width), BF16),
                pltpu.VMEM((seq_n, width), BF16),
                pltpu.VMEM((3, seq_n, width), BF16),
                pltpu.VMEM((seq_n, width), BF16),
                pltpu.VMEM((seq_n, width), BF16),
                pltpu.VMEM((seq_n, width), F32),
                pltpu.VMEM((2, seq_n, width), BF16),
                pltpu.VMEM((seq_n, seq_n), F32),
                pltpu.VMEM((2, 4, seq_n // 2, seq_n), F32),
                pltpu.VMEM((2, 4, seq_n // 2, seq_n), BF16),
                pltpu.VMEM((seq_n, width), BF16),
                pltpu.VMEM((4, width, width), BF16),
                pltpu.SemaphoreType.DMA((5,)),
                pltpu.SemaphoreType.DMA((pieces_n,)),
                pltpu.SemaphoreType.DMA((pieces_n,)),
                pltpu.SemaphoreType.DMA((pieces_n,)),
                pltpu.SemaphoreType.DMA((pieces_n,)),
                pltpu.SemaphoreType.DMA((units,)),
                pltpu.SemaphoreType.DMA((2, units)),
                pltpu.SemaphoreType.DMA((4, 2)),
                pltpu.SemaphoreType.DMA((2,)),
                pltpu.SemaphoreType.DMA,
                pltpu.SemaphoreType.DMA((2,)),
                pltpu.SemaphoreType.DMA((2,)),
                pltpu.SemaphoreType.DMA((2,)),
                pltpu.SemaphoreType.DMA((2,)),
            ],
            compiler_params=pltpu.CompilerParams(collective_id=0, has_side_effects=True, vmem_limit_bytes=63 * 1024 * 1024),
            cost_estimate=pl.CostEstimate(flops=flops, bytes_accessed=1 << 31, transcendentals=0),
            name='stage_kernel',
        )(x_in.reshape(total, seq_n, width), seq_lens.reshape(total), slopes, packed, *weights)
        return outs[0].reshape((1,) + x_in.shape)

    return jax.shard_map(per_device, mesh=mesh, in_specs=in_specs, out_specs=P('pp', 'dp'), check_vma=False)
```

```python
import functools
import math

import jax
import jax.numpy as jnp
import numpy as np
from jax import lax
from jax.experimental import pallas as pl
from jax.experimental.pallas import tpu as pltpu
from jax.sharding import PartitionSpec as P

MESH = pl.DeviceIdType.MESH
LOG2E = math.log2(math.e)
MASKED = -1e34
F32 = jnp.float32
BF16 = jnp.bfloat16
LN1_G, LN1_S, B_OUT, LN2_G, LN2_S, B_DOWN, B_QKV, B_UP = 0, 2, 4, 6, 8, 10, 12, 15


def alibi_slopes(heads_n):
    closest = 2 ** int(math.floor(math.log2(heads_n)))
    base_rate = 2.0 ** (-8.0 / closest)
    slope_list = [base_rate ** (head_idx + 1) for head_idx in range(closest)]
    extra_rate = 2.0 ** (-4.0 / closest)
    return slope_list + [extra_rate ** (2 * head_idx + 1) for head_idx in range(min(closest, heads_n - closest))]


def normalize(val_f, gain, shift):
    width = val_f.shape[-1]
    mean_val = jnp.sum(val_f, axis=-1, keepdims=True) * (1.0 / width)
    centered = val_f - mean_val
    var_val = jnp.sum(centered * centered, axis=-1, keepdims=True) * (1.0 / width)
    normed = centered * lax.rsqrt(var_val + 1e-5)
    return (normed * gain + shift).astype(BF16)


def gelu(val):
    inner = val * (0.7978845608028654 + (0.7978845608028654 * 0.044715) * (val * val))
    half = 0.5 * val
    return half + half * jnp.tanh(inner)


def stage_kernel(
    units, head_dim,
    x_hbm, lens, slopes, small_hbm, wqkv, wout, wup, wdown,
    hidden, inbox, ostage, wa_qkv, wa_out, wa_up, wa_down, wb_qkv, wb_out, wb_up, wb_down,
    small, x_buf, a_buf, qkv_buf, ctx_buf, h_buf, acc, u_buf, bias, score_buf, prob_buf, out_buf, ring,
    small_sem, wa_recv, wb_recv, w_send, w_fwd, in_recv, st_recv, ring_sem, x_sem, l_sem,
    y_send, c_send, x_send, f_send,
):
    dp = lax.axis_index('dp')
    y = lax.axis_index('tp')
    pp = lax.axis_index('pp')
    core = lax.rem(pp, 2)
    chip_x = pp // 2
    odd = lax.rem(chip_x + y, 2)
    stage = 2 * chip_x + odd
    own = core == odd
    not_own = core != odd
    is_odd = odd == 1
    is_even = odd == 0
    partner = (dp, y, 2 * chip_x + 1 - core)
    y_peer = (dp, 1 - y, pp)
    y_store = (dp, 1 - y, 2 * chip_x + 1)
    y_other = (dp, 1 - y, 2 * chip_x + 1 - core)
    x_peer = (dp, y, lax.rem(pp + 2, 4))
    seq_n, width = a_buf.shape
    half_w = wout.shape[0]
    heads_loc = half_w // head_dim
    parts = wup.shape[1] // width
    chunks = 2 * parts

    barrier = pltpu.get_barrier_semaphore()
    for other in (partner, y_peer, y_other, x_peer):
        pl.semaphore_signal(barrier, inc=1, device_id=other, device_id_type=MESH)
    pl.semaphore_wait(barrier, 4)

    def remote(src, dst, send_sem, recv_sem, device):
        return pltpu.make_async_remote_copy(src_ref=src, dst_ref=dst, send_sem=send_sem, recv_sem=recv_sem, device_id=device, device_id_type=MESH)

    def wait_on(ref, sem):
        pltpu.make_async_copy(ref, ref, sem).wait()

    def pieces(qkv, out, up, down, up_cut):
        found = [qkv.at[j] for j in range(3)] + [out]
        for m in range(parts):
            found.append(up.at[:, pl.ds(m * width, width)] if up_cut else up.at[m])
            found.append(down.at[pl.ds(m * width, width), :])
        return found

    mine = pieces(wqkv, wout, wup, wdown, True)
    got_a = pieces(wa_qkv, wa_out, wa_up, wa_down, False)
    got_b = pieces(wb_qkv, wb_out, wb_up, wb_down, False)
    pieces_n = len(mine)

    small_local = pltpu.make_async_copy(small_hbm, small.at[0], small_sem.at[0])
    small_give = remote(small_hbm, small.at[0], small_sem.at[1], small_sem.at[2], partner)
    small_cross = remote(small_hbm, small.at[1], small_sem.at[1], small_sem.at[3], y_peer)
    small_pass = remote(small.at[1], small.at[1], small_sem.at[4], small_sem.at[3], partner)

    @pl.when(own)
    def _():
        small_local.start()
        small_give.start()
        for j in range(pieces_n):
            remote(mine[j], got_a[j], w_send.at[j], wa_recv.at[j], partner).start()

    @pl.when(not_own)
    def _():
        small_cross.start()
        for j in range(pieces_n):
            remote(mine[j], got_b[j], w_send.at[j], wb_recv.at[j], y_peer).start()

    def pass_on(j):
        return remote(got_b[j], got_b[j], w_fwd.at[j], wb_recv.at[j], partner)

    def arrive_a(j):
        pl.when(not_own)(lambda: wait_on(got_a[j], wa_recv.at[j]))

    def arrive_b(j):
        wait_on(got_b[j], wb_recv.at[j])
        pl.when(own if j < pieces_n - 1 else own & (stage > 0))(lambda: pass_on(j).start())

    def slabs(src, dst, sems):
        rows = dst.shape[0] // len(sems)
        return [pltpu.make_async_copy(src.at[pl.ds(k * rows, rows), :], dst.at[pl.ds(k * rows, rows), :], sem) for k, sem in enumerate(sems)]

    def copy_a(j, dst, sems):
        @pl.when(own)
        def _():
            for copy in slabs(mine[j], dst, sems):
                copy.start()

        @pl.when(not_own)
        def _():
            for copy in slabs(got_a[j], dst, sems):
                copy.start()

    def copy_b(j, dst, sems):
        for copy in slabs(got_b[j], dst, sems):
            copy.start()

    tiles_n = 4 + 2 * chunks
    ring_n = ring.shape[0]

    def load_tile(p, first=None):
        p = p % tiles_n
        slot = p % ring_n
        if p < 4:
            left = ring.at[slot, :, pl.ds(0, half_w)] if p < 3 else ring.at[slot, pl.ds(0, half_w), :]
            right = ring.at[slot, :, pl.ds(half_w, half_w)] if p < 3 else ring.at[slot, pl.ds(half_w, half_w), :]
            if first is not None:
                @pl.when(first)
                def _():
                    arrive_a(p)
                    arrive_b(p)
            copy_a(p, left, [ring_sem.at[slot, k] for k in range(2)])
            copy_b(p, right, [ring_sem.at[slot, k] for k in range(2, 4)])
        else:
            m, is_down = (p - 4) // 2, (p - 4) % 2
            j = 4 + 2 * (m % parts) + is_down
            arrive, copy = (arrive_a, copy_a) if m < parts else (arrive_b, copy_b)
            if first is not None:
                pl.when(first)(lambda: arrive(j))
            copy(j, ring.at[slot], [ring_sem.at[slot, k] for k in range(4)])

    def wait_slot(slot):
        quarter = width // 4
        for k in range(4):
            wait_on(ring.at[slot, pl.ds(k * quarter, quarter), :], ring_sem.at[slot, k])

    def wait_tile(p):
        wait_slot(p % ring_n)

    half_n = seq_n // 2

    def place(p):
        return 2 * p + core, lax.rem(p, 2)

    def passed_on(p):
        seq, slot = place(p)
        return remote(inbox.at[p], hidden.at[seq], f_send.at[slot], st_recv.at[0, p], partner)

    def load_x(p):
        seq, slot = place(p)
        dst, sem = x_buf.at[slot], x_sem.at[slot]

        @pl.when(stage == 0)
        def _():
            pltpu.make_async_copy(x_hbm.at[seq], dst, sem).start()

        @pl.when(stage > 0)
        def _():
            wait_on(inbox.at[p], in_recv.at[p])

            @pl.when(is_odd & not_own)
            def _():
                pltpu.make_async_copy(hidden.at[seq], dst, sem).start()

            @pl.when(is_even | own)
            def _():
                pltpu.make_async_copy(inbox.at[p], dst, sem).start()

            @pl.when(is_odd & own)
            def _():
                pl.when(p >= 2)(lambda: passed_on(p - 2).wait_send())
                passed_on(p).start()

    def sends(p, src):
        seq, slot = place(p)
        return [
            (is_even & own, remote(src, hidden.at[seq], y_send.at[slot], in_recv.at[p], y_peer)),
            (is_even & not_own, remote(src, inbox.at[p], y_send.at[slot], in_recv.at[p], y_peer)),
            (stage == 1, remote(src, inbox.at[p], x_send.at[slot], in_recv.at[p], x_peer)),
            (is_odd, remote(src, hidden.at[seq], y_send.at[slot], st_recv.at[core, p], y_store)),
            (not_own, remote(src, hidden.at[seq], c_send.at[slot], st_recv.at[0, p], partner)),
        ]

    def each_send(p, what):
        @pl.when(own)
        def _():
            for cond, copy in sends(p, hidden.at[2 * p + core]):
                pl.when(cond)(functools.partial(what, copy))

        @pl.when(not_own)
        def _():
            for cond, copy in sends(p, ostage.at[p]):
                pl.when(cond)(functools.partial(what, copy))

    def store_out(p):
        pl.when(own)(lambda: pltpu.make_async_copy(out_buf, hidden.at[2 * p + core], l_sem).start())
        pl.when(not_own)(lambda: pltpu.make_async_copy(out_buf, ostage.at[p], l_sem).start())

    def start_sends(p):
        wait_on(out_buf, l_sem)
        pl.when(p >= 2)(lambda: each_send(p - 2, lambda copy: copy.wait_send()))
        each_send(p, lambda copy: copy.start())

    def wide(row):
        return jnp.concatenate([small[0, row:row + 1, :], small[0, row + 1:row + 2, :]], axis=-1)

    lane_tile = 128
    group_w = 384
    group_heads = group_w // head_dim
    groups_loc = heads_loc // group_heads
    spans = []
    for r in range(group_heads):
        low, high = r * head_dim, (r + 1) * head_dim
        start, stop = low // lane_tile * lane_tile, -(-high // lane_tile) * lane_tile
        spans.append((start, stop - start, low - start, high - start))
    q_rows = seq_n // 2
    sub = 16
    score_scale = head_dim ** -0.5 * LOG2E

    def scores(g):
        for qb in range(2):
            keys = (qb + 1) * q_rows
            for r, (start, span, low, high) in enumerate(spans):
                col = pl.ds(g * group_w + start, span)
                lane = lax.broadcasted_iota(jnp.int32, (keys, span), 1)
                k_val = qkv_buf[1, pl.ds(0, keys), col]
                k_val = jnp.where((lane >= low) & (lane < high), k_val, jnp.zeros_like(k_val))
                q_val = qkv_buf[0, pl.ds(qb * q_rows, q_rows), col]
                score_buf[qb, r, :, pl.ds(0, keys)] = lax.dot_general(q_val, k_val, (((1,), (1,)), ((), ())), preferred_element_type=F32)

    def soften(g):
        head = (y if g < groups_loc else 1 - y) * heads_loc + g % groups_loc * group_heads
        for qb in range(2):
            keys = (qb + 1) * q_rows
            for r in range(group_heads):
                slope = slopes[head + r]
                for blk in range(q_rows // sub):
                    rows = pl.ds(blk * sub, sub)
                    at = qb * q_rows + blk * sub
                    need = -(-(at + sub) // lane_tile) * lane_tile
                    score = score_buf[qb, r, rows, pl.ds(0, need)] * score_scale + slope * bias[pl.ds(at, sub), pl.ds(0, need)]
                    top = jnp.max(score, axis=-1, keepdims=True)
                    prob = jnp.exp2(score - top)
                    inv = 1.0 / jnp.sum(prob, axis=-1, keepdims=True)
                    prob_buf[qb, r, rows, pl.ds(0, need)] = (prob * inv).astype(BF16)
                    if need < keys:
                        prob_buf[qb, r, rows, pl.ds(need, keys - need)] = jnp.zeros((sub, keys - need), BF16)

    def contexts(g):
        lane = lax.broadcasted_iota(jnp.int32, (q_rows, lane_tile), 1)
        for qb in range(2):
            keys = (qb + 1) * q_rows
            outs = []
            for r, (start, span, low, high) in enumerate(spans):
                v_val = qkv_buf[2, pl.ds(0, keys), pl.ds(g * group_w + start, span)]
                outs.append(jnp.dot(prob_buf[qb, r, :, pl.ds(0, keys)], v_val, preferred_element_type=F32))
            for tile in range(group_w // lane_tile):
                value = None
                for r, (start, span, low, high) in enumerate(spans):
                    at = tile * lane_tile - start
                    if at < 0 or at >= span:
                        continue
                    piece = outs[r][:, at:at + lane_tile]
                    value = piece if value is None else jnp.where(lane >= low - at, piece, value)
                ctx_buf[pl.ds(qb * q_rows, q_rows), pl.ds(g * group_w + tile * lane_tile, lane_tile)] = value.astype(BF16)

    at_start = stage == 0

    @pl.when(stage > 0)
    def _():
        for j in range(pieces_n):
            arrive_a(j)
        for j in range(pieces_n):
            arrive_b(j)

    load_x(jnp.int32(0))
    for p in range(ring_n):
        load_tile(p, at_start)

    @pl.when(own)
    def _():
        small_local.wait()
        wait_on(small.at[1], small_sem.at[3])
        small_pass.start()

    @pl.when(not_own)
    def _():
        wait_on(small.at[0], small_sem.at[2])
        wait_on(small.at[1], small_sem.at[3])

    whole = pl.ds(0, seq_n)
    two = [pl.ds(k * half_n, half_n) for k in range(2)]

    def one_unit(p, carry):
        seq, slot = place(p)
        first = at_start & (p == 0)
        more = p + 1 < units
        wait_on(x_buf.at[slot], x_sem.at[slot])
        length = lens[seq]

        def bias_block(blk, carry):
            block = 64
            rows = pl.multiple_of(blk * block, block)
            query_pos = rows + lax.broadcasted_iota(jnp.int32, (block, seq_n), 0)
            key_pos = lax.broadcasted_iota(jnp.int32, (block, seq_n), 1)
            allowed = (key_pos <= query_pos) & (key_pos < length)
            bias[pl.ds(rows, block), :] = jnp.where(allowed, (key_pos - query_pos).astype(F32), MASKED)
            return carry

        lax.fori_loop(0, seq_n // 64, bias_block, 0)
        gain1, shift1 = wide(LN1_G), wide(LN1_S)

        def first_norm(low):
            for at in range(low, low + half_n, 16):
                a_buf[at:at + 16, :] = normalize(x_buf[slot, at:at + 16, :].astype(F32), gain1, shift1)

        def project(j, start, size, rows=whole):
            both = jnp.concatenate([small[k, B_QKV + j:B_QKV + j + 1, :] for k in range(2)], axis=-1)
            value = jnp.dot(a_buf[rows, :], ring[j, :, pl.ds(start, size)], preferred_element_type=F32)
            qkv_buf[j, rows, pl.ds(start, size)] = (value + both[:, start:start + size]).astype(BF16)

        def out_part(k_low, k_size, low, size):
            part = pl.ds(k_low, k_size)
            acc[:, pl.ds(low, size)] = jnp.dot(ctx_buf[:, part], ring[3, part, pl.ds(low, size)], preferred_element_type=F32)

        bias_out, bias_down, gain2, shift2 = wide(B_OUT), wide(B_DOWN), wide(LN2_G), wide(LN2_S)

        def add_attended(rows):
            resid = (x_buf[slot, rows, :].astype(F32) + acc[rows, :] + jnp.dot(ctx_buf[rows, half_w:], ring[3, half_w:, :], preferred_element_type=F32) + bias_out).astype(BF16)
            h_buf[rows, :] = resid
            acc[rows, :] = resid.astype(F32) + bias_down

        def second_norm(low):
            for at in range(low, low + half_n, 16):
                a_buf[at:at + 16, :] = normalize(h_buf[at:at + 16, :].astype(F32), gain2, shift2)

        def up(m, rows=whole):
            row = B_UP + 2 * lax.rem(m, parts)
            part = m // parts
            both = jnp.concatenate([small[part, pl.ds(row + k, 1), :] for k in range(2)], axis=-1)
            value = jnp.dot(a_buf[rows, :], ring[2 * lax.rem(m, 2)], preferred_element_type=F32) + both
            u_buf[lax.rem(m, 2), rows, :] = gelu(value).astype(BF16)

        def down(m):
            return jnp.dot(u_buf[lax.rem(m, 2)], ring[2 * lax.rem(m, 2) + 1], preferred_element_type=F32)

        cut = 2 * width // 3
        first_norm(0)
        pl.when(p > 0)(lambda: start_sends(p - 1))
        pl.when((stage == 0) & own & (p == 1))(lambda: pass_on(pieces_n - 1).start())
        for j in range(3):
            wait_tile(j)
        project(0, 0, cut, two[0])
        first_norm(half_n)
        project(0, 0, cut, two[1])
        project(1, 0, cut)
        project(2, 0, cut)
        scores(0)
        project(0, cut, width - cut)
        soften(0)
        scores(1)
        contexts(0)
        project(1, cut, width - cut)
        soften(1)
        project(2, cut, width - cut)
        contexts(1)
        for t in (4, 5, 6):
            load_tile(t, first)
        for t in (3, 4):
            wait_tile(t)
        scores(2)
        out_part(0, half_w, 0, cut)
        soften(2)
        scores(3)
        contexts(2)
        out_part(0, half_w, cut, width - cut)
        soften(3)
        contexts(3)
        for rows in two:
            add_attended(rows)
        second_norm(0)
        up(0, two[0])
        second_norm(half_n)
        up(0, two[1])
        load_tile(7, first)
        load_tile(8, first)

        def mlp(m, carry):
            up_slot, down_slot = 2 * lax.rem(m + 1, 2), 2 * lax.rem(m, 2) + 1
            wait_slot(up_slot)
            wait_slot(down_slot)
            up(m + 1)
            acc[...] += down(m)
            for at in range(chunks - 1):
                @pl.when(m == at)
                def _(at=at):
                    for t in (10 + 2 * at, 9 + 2 * at):
                        if t < tiles_n:
                            load_tile(t, first)
                        else:
                            pl.when(more)(functools.partial(load_tile, t))
            return carry

        lax.fori_loop(0, chunks - 1, mlp, 0)
        pl.when(more)(lambda: load_x(p + 1))
        wait_tile(11)
        out_buf[...] = (acc[...] + down(chunks - 1)).astype(BF16)
        pl.when(more)(functools.partial(load_tile, tiles_n + 3))
        store_out(p)
        return carry

    lax.fori_loop(0, units, one_unit, 0)
    start_sends(jnp.int32(units - 1))

    def settle(n, carry):
        p = units - 2 + n
        each_send(p, lambda copy: copy.wait_send())
        pl.when(is_odd & own)(lambda: passed_on(p).wait_send())
        return carry

    lax.fori_loop(0, 2, settle, 0)

    for j in range(pieces_n):
        wait_on(mine[j], w_send.at[j])
        pl.when(own)(lambda j=j: pass_on(j).wait_send())
    wait_on(small_hbm, small_sem.at[1])
    pl.when(own)(lambda: small_pass.wait_send())

    def drain(p, carry):
        wait_on(hidden.at[p], st_recv.at[0, p])
        pl.when(is_even & not_own)(lambda: wait_on(hidden.at[p], st_recv.at[1, p]))
        return carry

    lax.fori_loop(0, units, drain, 0)


def solution(mesh):
    in_specs = (P('dp'), P('dp'), P('pp'), P('pp'), P('pp', None, None, 'tp'), P('pp', None, 'tp', None), P('pp', 'tp', None), P('pp'), P('pp'), P('pp'), P('pp', None, 'tp'), P('pp', 'tp'), P('pp', 'tp', None), P('pp'))

    def per_device(x_in, seq_lens, ln1_gain, ln1_shift, w_qkv, b_qkv, w_out, b_out, ln2_gain, ln2_shift, w_up, b_up, w_down, b_down):
        micro_n, batch_n, seq_n, width = x_in.shape
        total = micro_n * batch_n
        units = total // 2
        half_w = w_out.shape[1]
        head_dim = b_qkv.shape[3]
        heads_n = width // head_dim
        up_w = w_up.shape[2]
        parts = up_w // width
        packed = jnp.concatenate([v[0].reshape(-1) for v in (ln1_gain, ln1_shift, b_out, ln2_gain, ln2_shift, b_down, b_qkv, b_up)])
        packed = packed.astype(F32).reshape(-1, half_w)
        packed = jnp.pad(packed, ((0, -packed.shape[0] % 8), (0, 0)))
        slopes = jnp.asarray(np.array(alibi_slopes(heads_n), np.float32) * np.float32(LOG2E))
        wqkv = jnp.transpose(w_qkv[0], (1, 0, 2))
        weights = (wqkv, w_out[0], w_up[0], w_down[0])
        hbm = pl.BlockSpec(memory_space=pl.ANY)
        smem = pl.BlockSpec(memory_space=pltpu.SMEM)
        seq_t = lambda n: jax.ShapeDtypeStruct((n, seq_n, width), BF16)
        half_t = [
            jax.ShapeDtypeStruct(wqkv.shape, BF16),
            jax.ShapeDtypeStruct((half_w, width), BF16),
            jax.ShapeDtypeStruct((parts, width, width), BF16),
            jax.ShapeDtypeStruct((up_w, width), BF16),
        ]
        pieces_n = 4 + 2 * parts
        flops = 2 * units * seq_n * width * (4 * width + 4 * up_w)
        outs = pl.pallas_call(
            functools.partial(stage_kernel, units, head_dim),
            out_shape=[seq_t(total), seq_t(units), seq_t(units)] + half_t + half_t,
            in_specs=[hbm, smem, smem, hbm] + [hbm] * 4,
            out_specs=[hbm] * 11,
            scratch_shapes=[
                pltpu.VMEM((2,) + packed.shape, F32),
                pltpu.VMEM((2, seq_n, width), BF16),
                pltpu.VMEM((seq_n, width), BF16),
                pltpu.VMEM((3, seq_n, width), BF16),
                pltpu.VMEM((seq_n, width), BF16),
                pltpu.VMEM((seq_n, width), BF16),
                pltpu.VMEM((seq_n, width), F32),
                pltpu.VMEM((2, seq_n, width), BF16),
                pltpu.VMEM((seq_n, seq_n), F32),
                pltpu.VMEM((2, 4, seq_n // 2, seq_n), F32),
                pltpu.VMEM((2, 4, seq_n // 2, seq_n), BF16),
                pltpu.VMEM((seq_n, width), BF16),
                pltpu.VMEM((4, width, width), BF16),
                pltpu.SemaphoreType.DMA((5,)),
                pltpu.SemaphoreType.DMA((pieces_n,)),
                pltpu.SemaphoreType.DMA((pieces_n,)),
                pltpu.SemaphoreType.DMA((pieces_n,)),
                pltpu.SemaphoreType.DMA((pieces_n,)),
                pltpu.SemaphoreType.DMA((units,)),
                pltpu.SemaphoreType.DMA((2, units)),
                pltpu.SemaphoreType.DMA((4, 4)),
                pltpu.SemaphoreType.DMA((2,)),
                pltpu.SemaphoreType.DMA,
                pltpu.SemaphoreType.DMA((2,)),
                pltpu.SemaphoreType.DMA((2,)),
                pltpu.SemaphoreType.DMA((2,)),
                pltpu.SemaphoreType.DMA((2,)),
            ],
            compiler_params=pltpu.CompilerParams(collective_id=0, has_side_effects=True, vmem_limit_bytes=63 * 1024 * 1024),
            cost_estimate=pl.CostEstimate(flops=flops, bytes_accessed=1 << 31, transcendentals=0),
            name='stage_kernel',
        )(x_in.reshape(total, seq_n, width), seq_lens.reshape(total), slopes, packed, *weights)
        return outs[0].reshape((1,) + x_in.shape)

    return jax.shard_map(per_device, mesh=mesh, in_specs=in_specs, out_specs=P('pp', 'dp'), check_vma=False)
```

```python
import functools
import math

import jax
import jax.numpy as jnp
import numpy as np
from jax import lax
from jax.experimental import pallas as pl
from jax.experimental.pallas import tpu as pltpu
from jax.sharding import PartitionSpec as P

MESH = pl.DeviceIdType.MESH
LOG2E = math.log2(math.e)
MASKED = -1e34
F32 = jnp.float32
BF16 = jnp.bfloat16
LN1_G, LN1_S, B_OUT, LN2_G, LN2_S, B_DOWN, B_QKV, B_UP = 0, 2, 4, 6, 8, 10, 12, 15


def alibi_slopes(heads_n):
    closest = 2 ** int(math.floor(math.log2(heads_n)))
    base_rate = 2.0 ** (-8.0 / closest)
    slope_list = [base_rate ** (head_idx + 1) for head_idx in range(closest)]
    extra_rate = 2.0 ** (-4.0 / closest)
    return slope_list + [extra_rate ** (2 * head_idx + 1) for head_idx in range(min(closest, heads_n - closest))]


def normalize(val_f, gain, shift):
    width = val_f.shape[-1]
    mean_val = jnp.sum(val_f, axis=-1, keepdims=True) * (1.0 / width)
    centered = val_f - mean_val
    var_val = jnp.sum(centered * centered, axis=-1, keepdims=True) * (1.0 / width)
    normed = centered * lax.rsqrt(var_val + 1e-5)
    return (normed * gain + shift).astype(BF16)


def gelu(val):
    inner = val * (0.7978845608028654 + (0.7978845608028654 * 0.044715) * (val * val))
    half = 0.5 * val
    return half + half * jnp.tanh(inner)


def stage_kernel(
    units, head_dim,
    x_hbm, lens, slopes, small_hbm, wqkv, wout, wup, wdown,
    hidden, inbox, ostage, relay, wa_qkv, wa_out, wa_up, wa_down, wb_qkv, wb_out, wb_up, wb_down,
    small, x_buf, a_buf, qkv_buf, ctx_buf, h_buf, acc, u_buf, bias, score_buf, prob_buf, out_buf, ring,
    small_sem, wa_recv, wb_recv, w_send, w_fwd, r_send, r_recv, in_recv, st_recv, ring_sem, x_sem, l_sem,
    y_send, c_send, x_send, f_send,
):
    dp = lax.axis_index('dp')
    y = lax.axis_index('tp')
    pp = lax.axis_index('pp')
    core = lax.rem(pp, 2)
    chip_x = pp // 2
    odd = lax.rem(chip_x + y, 2)
    stage = 2 * chip_x + odd
    own = core == odd
    not_own = core != odd
    is_odd = odd == 1
    is_even = odd == 0
    partner = (dp, y, 2 * chip_x + 1 - core)
    y_peer = (dp, 1 - y, pp)
    y_store = (dp, 1 - y, 2 * chip_x + 1)
    y_other = (dp, 1 - y, 2 * chip_x + 1 - core)
    x_peer = (dp, y, lax.rem(pp + 2, 4))
    x_diag = (dp, y, 3 - pp)
    is_origin = (pp == 0) & (y == 1)
    is_turn = (pp == 3) & (y == 1)
    is_last = (pp == 3) & (y == 0)
    is_goal = (pp == 0) & (y == 0)
    seq_n, width = a_buf.shape
    half_w = wout.shape[0]
    heads_loc = half_w // head_dim
    parts = wup.shape[1] // width
    chunks = 2 * parts

    barrier = pltpu.get_barrier_semaphore()
    for other in (partner, y_peer, y_other, x_peer, x_diag):
        pl.semaphore_signal(barrier, inc=1, device_id=other, device_id_type=MESH)
    pl.semaphore_wait(barrier, 5)

    def remote(src, dst, send_sem, recv_sem, device):
        return pltpu.make_async_remote_copy(src_ref=src, dst_ref=dst, send_sem=send_sem, recv_sem=recv_sem, device_id=device, device_id_type=MESH)

    def wait_on(ref, sem):
        pltpu.make_async_copy(ref, ref, sem).wait()

    def pieces(qkv, out, up, down, up_cut):
        found = [qkv.at[j] for j in range(3)] + [out]
        for m in range(parts):
            found.append(up.at[:, pl.ds(m * width, width)] if up_cut else up.at[m])
            found.append(down.at[pl.ds(m * width, width), :])
        return found

    mine = pieces(wqkv, wout, wup, wdown, True)
    got_a = pieces(wa_qkv, wa_out, wa_up, wa_down, False)
    got_b = pieces(wb_qkv, wb_out, wb_up, wb_down, False)
    pieces_n = len(mine)

    small_local = pltpu.make_async_copy(small_hbm, small.at[0], small_sem.at[0])
    small_give = remote(small_hbm, small.at[0], small_sem.at[1], small_sem.at[2], partner)
    small_cross = remote(small_hbm, small.at[1], small_sem.at[1], small_sem.at[3], y_peer)
    small_pass = remote(small.at[1], small.at[1], small_sem.at[4], small_sem.at[3], partner)

    @pl.when(own)
    def _():
        small_local.start()
        small_give.start()
        for j in range(pieces_n):
            remote(mine[j], got_a[j], w_send.at[j], wa_recv.at[j], partner).start()

    relays_n = relay.shape[0]
    relay_rows = relay.shape[1]

    def relay_part(ref, k):
        return ref.at[pl.ds(k * relay_rows, relay_rows), :]

    def relayed(j):
        return j >= 4 and j % 2 == 1

    def give_away(k):
        return remote(relay_part(wdown, k), relay.at[k], r_send.at[k], r_recv.at[k], x_diag)

    def turn(k):
        return remote(relay.at[k], relay.at[k], r_send.at[k], r_recv.at[k], y_peer)

    def deliver(k):
        return remote(relay.at[k], relay_part(wb_down, k), r_send.at[k], r_recv.at[k], x_diag)

    @pl.when(not_own)
    def _():
        small_cross.start()

        @pl.when(is_origin)
        def _():
            for k in range(relays_n):
                give_away(k).start()

        @pl.when(is_turn)
        def _():
            for k in range(relays_n):
                wait_on(relay.at[k], r_recv.at[k])
                turn(k).start()
        for j in range(pieces_n):
            cross = remote(mine[j], got_b[j], w_send.at[j], wb_recv.at[j], y_peer)
            pl.when(jnp.logical_not(is_origin) if relayed(j) else not_own)(lambda cross=cross: cross.start())

    @pl.when(is_last)
    def _():
        for k in range(relays_n):
            wait_on(relay.at[k], r_recv.at[k])
            deliver(k).start()

    def pass_on(j):
        return remote(got_b[j], got_b[j], w_fwd.at[j], wb_recv.at[j], partner)

    def arrive_a(j):
        pl.when(not_own)(lambda: wait_on(got_a[j], wa_recv.at[j]))

    def arrive_b(j):
        if relayed(j):
            @pl.when(is_goal)
            def _():
                each = relays_n // parts
                for k in range((j - 5) // 2 * each, ((j - 5) // 2 + 1) * each):
                    wait_on(relay.at[k], r_recv.at[k])
            pl.when(jnp.logical_not(is_goal))(lambda: wait_on(got_b[j], wb_recv.at[j]))
        else:
            wait_on(got_b[j], wb_recv.at[j])
        pl.when(own)(lambda: pass_on(j).start())

    def slabs(src, dst, sems):
        rows = dst.shape[0] // len(sems)
        return [pltpu.make_async_copy(src.at[pl.ds(k * rows, rows), :], dst.at[pl.ds(k * rows, rows), :], sem) for k, sem in enumerate(sems)]

    def copy_a(j, dst, sems):
        @pl.when(own)
        def _():
            for copy in slabs(mine[j], dst, sems):
                copy.start()

        @pl.when(not_own)
        def _():
            for copy in slabs(got_a[j], dst, sems):
                copy.start()

    def copy_b(j, dst, sems):
        for copy in slabs(got_b[j], dst, sems):
            copy.start()

    tiles_n = 4 + 2 * chunks
    ring_n = ring.shape[0]

    def load_tile(p, first=None):
        p = p % tiles_n
        slot = p % ring_n
        if p < 4:
            left = ring.at[slot, :, pl.ds(0, half_w)] if p < 3 else ring.at[slot, pl.ds(0, half_w), :]
            right = ring.at[slot, :, pl.ds(half_w, half_w)] if p < 3 else ring.at[slot, pl.ds(half_w, half_w), :]
            if first is not None:
                @pl.when(first[0])
                def _():
                    arrive_a(p)
                    arrive_b(p)
            copy_a(p, left, [ring_sem.at[slot, k] for k in range(2)])
            copy_b(p, right, [ring_sem.at[slot, k] for k in range(2, 4)])
        else:
            m, is_down = (p - 4) // 2, (p - 4) % 2
            j = 4 + 2 * (m % parts) + is_down
            arrive, copy = (arrive_a, copy_a) if m < parts else (arrive_b, copy_b)
            if first is not None:
                late = m >= parts and j >= pieces_n - 2
                pl.when((stage <= 1) & (first[1] == 0) if late else first[0])(lambda: arrive(j))
            copy(j, ring.at[slot], [ring_sem.at[slot, k] for k in range(4)])

    def wait_slot(slot):
        quarter = width // 4
        for k in range(4):
            wait_on(ring.at[slot, pl.ds(k * quarter, quarter), :], ring_sem.at[slot, k])

    def wait_tile(p):
        wait_slot(p % ring_n)

    half_n = seq_n // 2

    def place(p):
        return 2 * p + core, lax.rem(p, 2)

    def passed_on(p):
        seq, slot = place(p)
        return remote(inbox.at[p], hidden.at[seq], f_send.at[slot], st_recv.at[0, p], partner)

    def load_x(p):
        seq, slot = place(p)
        dst, sem = x_buf.at[slot], x_sem.at[slot]

        @pl.when(stage == 0)
        def _():
            pltpu.make_async_copy(x_hbm.at[seq], dst, sem).start()

        @pl.when(stage > 0)
        def _():
            wait_on(inbox.at[p], in_recv.at[p])

            @pl.when(is_odd & not_own)
            def _():
                pltpu.make_async_copy(hidden.at[seq], dst, sem).start()

            @pl.when(is_even | own)
            def _():
                pltpu.make_async_copy(inbox.at[p], dst, sem).start()

            @pl.when(is_odd & own)
            def _():
                pl.when(p >= 2)(lambda: passed_on(p - 2).wait_send())
                passed_on(p).start()

    def sends(p, src):
        seq, slot = place(p)
        return [
            (is_even & own, remote(src, hidden.at[seq], y_send.at[slot], in_recv.at[p], y_peer)),
            (is_even & not_own, remote(src, inbox.at[p], y_send.at[slot], in_recv.at[p], y_peer)),
            (stage == 1, remote(src, inbox.at[p], x_send.at[slot], in_recv.at[p], x_peer)),
            (is_odd, remote(src, hidden.at[seq], y_send.at[slot], st_recv.at[core, p], y_store)),
            (not_own, remote(src, hidden.at[seq], c_send.at[slot], st_recv.at[0, p], partner)),
        ]

    def each_send(p, what):
        @pl.when(own)
        def _():
            for cond, copy in sends(p, hidden.at[2 * p + core]):
                pl.when(cond)(functools.partial(what, copy))

        @pl.when(not_own)
        def _():
            for cond, copy in sends(p, ostage.at[p]):
                pl.when(cond)(functools.partial(what, copy))

    def store_out(p):
        pl.when(own)(lambda: pltpu.make_async_copy(out_buf, hidden.at[2 * p + core], l_sem).start())
        pl.when(not_own)(lambda: pltpu.make_async_copy(out_buf, ostage.at[p], l_sem).start())

    def start_sends(p):
        wait_on(out_buf, l_sem)
        pl.when(p >= 2)(lambda: each_send(p - 2, lambda copy: copy.wait_send()))
        each_send(p, lambda copy: copy.start())

    def wide(row):
        return jnp.concatenate([small[0, row:row + 1, :], small[0, row + 1:row + 2, :]], axis=-1)

    lane_tile = 128
    group_w = 384
    group_heads = group_w // head_dim
    groups_loc = heads_loc // group_heads
    spans = []
    for r in range(group_heads):
        low, high = r * head_dim, (r + 1) * head_dim
        start, stop = low // lane_tile * lane_tile, -(-high // lane_tile) * lane_tile
        spans.append((start, stop - start, low - start, high - start))
    q_rows = seq_n // 2
    sub = 16
    score_scale = head_dim ** -0.5 * LOG2E

    def scores(g):
        for qb in range(2):
            keys = (qb + 1) * q_rows
            for r, (start, span, low, high) in enumerate(spans):
                col = pl.ds(g * group_w + start, span)
                lane = lax.broadcasted_iota(jnp.int32, (keys, span), 1)
                k_val = qkv_buf[1, pl.ds(0, keys), col]
                k_val = jnp.where((lane >= low) & (lane < high), k_val, jnp.zeros_like(k_val))
                q_val = qkv_buf[0, pl.ds(qb * q_rows, q_rows), col]
                score_buf[qb, r, :, pl.ds(0, keys)] = lax.dot_general(q_val, k_val, (((1,), (1,)), ((), ())), preferred_element_type=F32)

    def soften(g):
        head = (y if g < groups_loc else 1 - y) * heads_loc + g % groups_loc * group_heads
        for qb in range(2):
            keys = (qb + 1) * q_rows
            for r in range(group_heads):
                slope = slopes[head + r]
                for blk in range(q_rows // sub):
                    rows = pl.ds(blk * sub, sub)
                    at = qb * q_rows + blk * sub
                    need = -(-(at + sub) // lane_tile) * lane_tile
                    score = score_buf[qb, r, rows, pl.ds(0, need)] * score_scale + slope * bias[pl.ds(at, sub), pl.ds(0, need)]
                    top = jnp.max(score, axis=-1, keepdims=True)
                    prob = jnp.exp2(score - top)
                    inv = 1.0 / jnp.sum(prob, axis=-1, keepdims=True)
                    prob_buf[qb, r, rows, pl.ds(0, need)] = (prob * inv).astype(BF16)
                    if need < keys:
                        prob_buf[qb, r, rows, pl.ds(need, keys - need)] = jnp.zeros((sub, keys - need), BF16)

    def contexts(g):
        lane = lax.broadcasted_iota(jnp.int32, (q_rows, lane_tile), 1)
        for qb in range(2):
            keys = (qb + 1) * q_rows
            outs = []
            for r, (start, span, low, high) in enumerate(spans):
                v_val = qkv_buf[2, pl.ds(0, keys), pl.ds(g * group_w + start, span)]
                outs.append(jnp.dot(prob_buf[qb, r, :, pl.ds(0, keys)], v_val, preferred_element_type=F32))
            for tile in range(group_w // lane_tile):
                value = None
                for r, (start, span, low, high) in enumerate(spans):
                    at = tile * lane_tile - start
                    if at < 0 or at >= span:
                        continue
                    piece = outs[r][:, at:at + lane_tile]
                    value = piece if value is None else jnp.where(lane >= low - at, piece, value)
                ctx_buf[pl.ds(qb * q_rows, q_rows), pl.ds(g * group_w + tile * lane_tile, lane_tile)] = value.astype(BF16)

    at_start = stage == 0

    @pl.when(stage > 0)
    def _():
        for j in range(pieces_n):
            arrive_a(j)
        for j in range(pieces_n - 2):
            arrive_b(j)

        @pl.when(stage > 1)
        def _():
            for j in range(pieces_n - 2, pieces_n):
                arrive_b(j)

    load_x(jnp.int32(0))
    for p in range(ring_n):
        load_tile(p, (at_start, 0))

    @pl.when(own)
    def _():
        small_local.wait()
        wait_on(small.at[1], small_sem.at[3])
        small_pass.start()

    @pl.when(not_own)
    def _():
        wait_on(small.at[0], small_sem.at[2])
        wait_on(small.at[1], small_sem.at[3])

    whole = pl.ds(0, seq_n)
    two = [pl.ds(k * half_n, half_n) for k in range(2)]

    def one_unit(p, carry):
        seq, slot = place(p)
        first = (at_start & (p == 0), p)
        more = p + 1 < units
        wait_on(x_buf.at[slot], x_sem.at[slot])
        length = lens[seq]

        def bias_block(blk, carry):
            block = 64
            rows = pl.multiple_of(blk * block, block)
            query_pos = rows + lax.broadcasted_iota(jnp.int32, (block, seq_n), 0)
            key_pos = lax.broadcasted_iota(jnp.int32, (block, seq_n), 1)
            allowed = (key_pos <= query_pos) & (key_pos < length)
            bias[pl.ds(rows, block), :] = jnp.where(allowed, (key_pos - query_pos).astype(F32), MASKED)
            return carry

        lax.fori_loop(0, seq_n // 64, bias_block, 0)
        gain1, shift1 = wide(LN1_G), wide(LN1_S)

        def first_norm(low):
            for at in range(low, low + half_n, 16):
                a_buf[at:at + 16, :] = normalize(x_buf[slot, at:at + 16, :].astype(F32), gain1, shift1)

        def project(j, start, size, rows=whole):
            both = jnp.concatenate([small[k, B_QKV + j:B_QKV + j + 1, :] for k in range(2)], axis=-1)
            value = jnp.dot(a_buf[rows, :], ring[j, :, pl.ds(start, size)], preferred_element_type=F32)
            qkv_buf[j, rows, pl.ds(start, size)] = (value + both[:, start:start + size]).astype(BF16)

        def out_part(k_low, k_size, low, size):
            part = pl.ds(k_low, k_size)
            acc[:, pl.ds(low, size)] = jnp.dot(ctx_buf[:, part], ring[3, part, pl.ds(low, size)], preferred_element_type=F32)

        bias_out, bias_down, gain2, shift2 = wide(B_OUT), wide(B_DOWN), wide(LN2_G), wide(LN2_S)

        def add_attended(rows):
            resid = (x_buf[slot, rows, :].astype(F32) + acc[rows, :] + jnp.dot(ctx_buf[rows, half_w:], ring[3, half_w:, :], preferred_element_type=F32) + bias_out).astype(BF16)
            h_buf[rows, :] = resid
            acc[rows, :] = resid.astype(F32) + bias_down

        def second_norm(low):
            for at in range(low, low + half_n, 16):
                a_buf[at:at + 16, :] = normalize(h_buf[at:at + 16, :].astype(F32), gain2, shift2)

        def up(m, rows=whole):
            row = B_UP + 2 * lax.rem(m, parts)
            part = m // parts
            both = jnp.concatenate([small[part, pl.ds(row + k, 1), :] for k in range(2)], axis=-1)
            value = jnp.dot(a_buf[rows, :], ring[2 * lax.rem(m, 2)], preferred_element_type=F32) + both
            u_buf[lax.rem(m, 2), rows, :] = gelu(value).astype(BF16)

        def down(m):
            return jnp.dot(u_buf[lax.rem(m, 2)], ring[2 * lax.rem(m, 2) + 1], preferred_element_type=F32)

        cut = 2 * width // 3
        first_norm(0)
        pl.when(p > 0)(lambda: start_sends(p - 1))
        for j in range(3):
            wait_tile(j)
        project(0, 0, cut, two[0])
        first_norm(half_n)
        project(0, 0, cut, two[1])
        project(1, 0, cut)
        project(2, 0, cut)
        scores(0)
        project(0, cut, width - cut)
        soften(0)
        scores(1)
        contexts(0)
        project(1, cut, width - cut)
        soften(1)
        project(2, cut, width - cut)
        contexts(1)
        for t in (4, 5, 6):
            load_tile(t, first)
        for t in (3, 4):
            wait_tile(t)
        scores(2)
        out_part(0, half_w, 0, cut)
        soften(2)
        scores(3)
        contexts(2)
        out_part(0, half_w, cut, width - cut)
        soften(3)
        contexts(3)
        for rows in two:
            add_attended(rows)
        second_norm(0)
        up(0, two[0])
        second_norm(half_n)
        up(0, two[1])
        load_tile(7, first)
        load_tile(8, first)

        def mlp(m, carry):
            up_slot, down_slot = 2 * lax.rem(m + 1, 2), 2 * lax.rem(m, 2) + 1
            wait_slot(up_slot)
            wait_slot(down_slot)
            up(m + 1)
            acc[...] += down(m)
            for at in range(chunks - 1):
                @pl.when(m == at)
                def _(at=at):
                    for t in (10 + 2 * at, 9 + 2 * at):
                        if t < tiles_n:
                            load_tile(t, first)
                        else:
                            pl.when(more)(functools.partial(load_tile, t))
            return carry

        lax.fori_loop(0, chunks - 1, mlp, 0)
        pl.when(more)(lambda: load_x(p + 1))
        wait_tile(11)
        out_buf[...] = (acc[...] + down(chunks - 1)).astype(BF16)
        pl.when(more)(functools.partial(load_tile, tiles_n + 3))
        store_out(p)
        return carry

    lax.fori_loop(0, units, one_unit, 0)
    start_sends(jnp.int32(units - 1))

    def settle(n, carry):
        p = units - 2 + n
        each_send(p, lambda copy: copy.wait_send())
        pl.when(is_odd & own)(lambda: passed_on(p).wait_send())
        return carry

    lax.fori_loop(0, 2, settle, 0)

    @pl.when(is_origin | is_turn | is_last)
    def _():
        for k in range(relays_n):
            wait_on(relay.at[k], r_send.at[k])

    for j in range(pieces_n):
        pl.when(jnp.logical_not(is_origin) if relayed(j) else pp >= 0)(lambda j=j: wait_on(mine[j], w_send.at[j]))
        pl.when(own)(lambda j=j: pass_on(j).wait_send())
    wait_on(small_hbm, small_sem.at[1])
    pl.when(own)(lambda: small_pass.wait_send())

    def drain(p, carry):
        wait_on(hidden.at[p], st_recv.at[0, p])
        pl.when(is_even & not_own)(lambda: wait_on(hidden.at[p], st_recv.at[1, p]))
        return carry

    lax.fori_loop(0, units, drain, 0)


def solution(mesh):
    in_specs = (P('dp'), P('dp'), P('pp'), P('pp'), P('pp', None, None, 'tp'), P('pp', None, 'tp', None), P('pp', 'tp', None), P('pp'), P('pp'), P('pp'), P('pp', None, 'tp'), P('pp', 'tp'), P('pp', 'tp', None), P('pp'))

    def per_device(x_in, seq_lens, ln1_gain, ln1_shift, w_qkv, b_qkv, w_out, b_out, ln2_gain, ln2_shift, w_up, b_up, w_down, b_down):
        micro_n, batch_n, seq_n, width = x_in.shape
        total = micro_n * batch_n
        units = total // 2
        half_w = w_out.shape[1]
        head_dim = b_qkv.shape[3]
        heads_n = width // head_dim
        up_w = w_up.shape[2]
        parts = up_w // width
        packed = jnp.concatenate([v[0].reshape(-1) for v in (ln1_gain, ln1_shift, b_out, ln2_gain, ln2_shift, b_down, b_qkv, b_up)])
        packed = packed.astype(F32).reshape(-1, half_w)
        packed = jnp.pad(packed, ((0, -packed.shape[0] % 8), (0, 0)))
        slopes = jnp.asarray(np.array(alibi_slopes(heads_n), np.float32) * np.float32(LOG2E))
        wqkv = jnp.transpose(w_qkv[0], (1, 0, 2))
        weights = (wqkv, w_out[0], w_up[0], w_down[0])
        hbm = pl.BlockSpec(memory_space=pl.ANY)
        smem = pl.BlockSpec(memory_space=pltpu.SMEM)
        seq_t = lambda n: jax.ShapeDtypeStruct((n, seq_n, width), BF16)
        half_t = [
            jax.ShapeDtypeStruct(wqkv.shape, BF16),
            jax.ShapeDtypeStruct((half_w, width), BF16),
            jax.ShapeDtypeStruct((parts, width, width), BF16),
            jax.ShapeDtypeStruct((up_w, width), BF16),
        ]
        pieces_n = 4 + 2 * parts
        flops = 2 * units * seq_n * width * (4 * width + 4 * up_w)
        outs = pl.pallas_call(
            functools.partial(stage_kernel, units, head_dim),
            out_shape=[seq_t(total), seq_t(units), seq_t(units), jax.ShapeDtypeStruct((8, up_w // 8, width), BF16)] + half_t + half_t,
            in_specs=[hbm, smem, smem, hbm] + [hbm] * 4,
            out_specs=[hbm] * 12,
            scratch_shapes=[
                pltpu.VMEM((2,) + packed.shape, F32),
                pltpu.VMEM((2, seq_n, width), BF16),
                pltpu.VMEM((seq_n, width), BF16),
                pltpu.VMEM((3, seq_n, width), BF16),
                pltpu.VMEM((seq_n, width), BF16),
                pltpu.VMEM((seq_n, width), BF16),
                pltpu.VMEM((seq_n, width), F32),
                pltpu.VMEM((2, seq_n, width), BF16),
                pltpu.VMEM((seq_n, seq_n), F32),
                pltpu.VMEM((2, 4, seq_n // 2, seq_n), F32),
                pltpu.VMEM((2, 4, seq_n // 2, seq_n), BF16),
                pltpu.VMEM((seq_n, width), BF16),
                pltpu.VMEM((4, width, width), BF16),
                pltpu.SemaphoreType.DMA((5,)),
                pltpu.SemaphoreType.DMA((pieces_n,)),
                pltpu.SemaphoreType.DMA((pieces_n,)),
                pltpu.SemaphoreType.DMA((pieces_n,)),
                pltpu.SemaphoreType.DMA((pieces_n,)),
                pltpu.SemaphoreType.DMA((8,)),
                pltpu.SemaphoreType.DMA((8,)),
                pltpu.SemaphoreType.DMA((units,)),
                pltpu.SemaphoreType.DMA((2, units)),
                pltpu.SemaphoreType.DMA((4, 4)),
                pltpu.SemaphoreType.DMA((2,)),
                pltpu.SemaphoreType.DMA,
                pltpu.SemaphoreType.DMA((2,)),
                pltpu.SemaphoreType.DMA((2,)),
                pltpu.SemaphoreType.DMA((2,)),
                pltpu.SemaphoreType.DMA((2,)),
            ],
            compiler_params=pltpu.CompilerParams(collective_id=0, has_side_effects=True, vmem_limit_bytes=63 * 1024 * 1024),
            cost_estimate=pl.CostEstimate(flops=flops, bytes_accessed=1 << 31, transcendentals=0),
            name='stage_kernel',
        )(x_in.reshape(total, seq_n, width), seq_lens.reshape(total), slopes, packed, *weights)
        return outs[0].reshape((1,) + x_in.shape)

    return jax.shard_map(per_device, mesh=mesh, in_specs=in_specs, out_specs=P('pp', 'dp'), check_vma=False)
```

```python
import functools
import math

import jax
import jax.numpy as jnp
import numpy as np
from jax import lax
from jax.experimental import pallas as pl
from jax.experimental.pallas import tpu as pltpu
from jax.sharding import PartitionSpec as P

MESH = pl.DeviceIdType.MESH
LOG2E = math.log2(math.e)
MASKED = -1e34
F32 = jnp.float32
BF16 = jnp.bfloat16
LN1_G, LN1_S, B_OUT, LN2_G, LN2_S, B_DOWN, B_QKV, B_UP = 0, 2, 4, 6, 8, 10, 12, 15


def alibi_slopes(heads_n):
    closest = 2 ** int(math.floor(math.log2(heads_n)))
    base_rate = 2.0 ** (-8.0 / closest)
    slope_list = [base_rate ** (head_idx + 1) for head_idx in range(closest)]
    extra_rate = 2.0 ** (-4.0 / closest)
    return slope_list + [extra_rate ** (2 * head_idx + 1) for head_idx in range(min(closest, heads_n - closest))]


def normalize(val_f, gain, shift):
    width = val_f.shape[-1]
    mean_val = jnp.sum(val_f, axis=-1, keepdims=True) * (1.0 / width)
    centered = val_f - mean_val
    var_val = jnp.sum(centered * centered, axis=-1, keepdims=True) * (1.0 / width)
    normed = centered * lax.rsqrt(var_val + 1e-5)
    return (normed * gain + shift).astype(BF16)


def gelu(val):
    inner = val * (0.7978845608028654 + (0.7978845608028654 * 0.044715) * (val * val))
    half = 0.5 * val
    return half + half * jnp.tanh(inner)


def pack_kernel(*refs):
    packed = refs[-1]
    wide = packed.shape[1]
    row = 0
    for ref in refs[:-1]:
        for low in range(0, ref.shape[1], wide):
            packed[row:row + 1, :] = ref[0:1, low:low + wide].astype(F32)
            row += 1
    packed[row:, :] = jnp.zeros((packed.shape[0] - row, wide), F32)


def stage_kernel(
    units, head_dim,
    x_hbm, lens, slopes, small_hbm, wqkv, wout, wup, wdown,
    hidden, inbox, ostage, wa_qkv, wa_out, wa_up, wa_down, wb_qkv, wb_out, wb_up, wb_down,
    small, x_buf, a_buf, qkv_buf, ctx_buf, h_buf, acc, u_buf, bias, score_buf, prob_buf, out_buf, ring,
    small_sem, wa_recv, wb_recv, w_send, w_fwd, in_recv, st_recv, ring_sem, x_sem, l_sem,
    y_send, c_send, x_send, f_send,
):
    dp = lax.axis_index('dp')
    y = lax.axis_index('tp')
    pp = lax.axis_index('pp')
    core = lax.rem(pp, 2)
    chip_x = pp // 2
    odd = lax.rem(chip_x + y, 2)
    stage = 2 * chip_x + odd
    own = core == odd
    not_own = core != odd
    is_odd = odd == 1
    is_even = odd == 0
    partner = (dp, y, 2 * chip_x + 1 - core)
    y_peer = (dp, 1 - y, pp)
    y_store = (dp, 1 - y, 2 * chip_x + 1)
    y_other = (dp, 1 - y, 2 * chip_x + 1 - core)
    x_peer = (dp, y, lax.rem(pp + 2, 4))
    seq_n, width = a_buf.shape
    half_w = wout.shape[0]
    heads_loc = half_w // head_dim
    parts = wup.shape[1] // width
    chunks = 2 * parts

    barrier = pltpu.get_barrier_semaphore()
    for other in (partner, y_peer, y_other, x_peer):
        pl.semaphore_signal(barrier, inc=1, device_id=other, device_id_type=MESH)
    pl.semaphore_wait(barrier, 4)

    def remote(src, dst, send_sem, recv_sem, device):
        return pltpu.make_async_remote_copy(src_ref=src, dst_ref=dst, send_sem=send_sem, recv_sem=recv_sem, device_id=device, device_id_type=MESH)

    def wait_on(ref, sem):
        pltpu.make_async_copy(ref, ref, sem).wait()

    def pieces(qkv, out, up, down, up_cut):
        found = [qkv.at[j] for j in range(3)] + [out]
        for m in range(parts):
            found.append(up.at[:, pl.ds(m * width, width)] if up_cut else up.at[m])
            found.append(down.at[pl.ds(m * width, width), :])
        return found

    mine = pieces(wqkv, wout, wup, wdown, True)
    got_a = pieces(wa_qkv, wa_out, wa_up, wa_down, False)
    got_b = pieces(wb_qkv, wb_out, wb_up, wb_down, False)
    pieces_n = len(mine)

    small_local = pltpu.make_async_copy(small_hbm, small.at[0], small_sem.at[0])
    small_give = remote(small_hbm, small.at[0], small_sem.at[1], small_sem.at[2], partner)
    small_cross = remote(small_hbm, small.at[1], small_sem.at[1], small_sem.at[3], y_peer)
    small_pass = remote(small.at[1], small.at[1], small_sem.at[4], small_sem.at[3], partner)

    @pl.when(own)
    def _():
        small_local.start()
        small_give.start()
        for j in range(pieces_n):
            remote(mine[j], got_a[j], w_send.at[j], wa_recv.at[j], partner).start()

    @pl.when(not_own)
    def _():
        small_cross.start()
        for j in range(pieces_n):
            remote(mine[j], got_b[j], w_send.at[j], wb_recv.at[j], y_peer).start()

    def pass_on(j):
        return remote(got_b[j], got_b[j], w_fwd.at[j], wb_recv.at[j], partner)

    def arrive_a(j):
        pl.when(not_own)(lambda: wait_on(got_a[j], wa_recv.at[j]))

    def arrive_b(j):
        wait_on(got_b[j], wb_recv.at[j])
        pl.when(own if j < pieces_n - 1 else own & (stage > 0))(lambda: pass_on(j).start())

    def copy_a(j, dst, sem):
        pl.when(own)(lambda: pltpu.make_async_copy(mine[j], dst, sem).start())
        pl.when(not_own)(lambda: pltpu.make_async_copy(got_a[j], dst, sem).start())

    def copy_b(j, dst, sem):
        pltpu.make_async_copy(got_b[j], dst, sem).start()

    tiles_n = 4 + 2 * chunks
    ring_n = ring.shape[0]

    def load_tile(p, first=None):
        p = p % tiles_n
        slot = p % ring_n
        if p < 4:
            left = ring.at[slot, :, pl.ds(0, half_w)] if p < 3 else ring.at[slot, pl.ds(0, half_w), :]
            right = ring.at[slot, :, pl.ds(half_w, half_w)] if p < 3 else ring.at[slot, pl.ds(half_w, half_w), :]
            if first is not None:
                @pl.when(first)
                def _():
                    arrive_a(p)
                    arrive_b(p)
            copy_a(p, left, ring_sem.at[slot, 0])
            copy_b(p, right, ring_sem.at[slot, 1])
        else:
            m, is_down = (p - 4) // 2, (p - 4) % 2
            j = 4 + 2 * (m % parts) + is_down
            arrive, copy = (arrive_a, copy_a) if m < parts else (arrive_b, copy_b)
            if first is not None:
                pl.when(first)(lambda: arrive(j))
            copy(j, ring.at[slot], ring_sem.at[slot, 0])

    def wait_tile(p):
        slot = p % ring_n
        if p < 4:
            for k in range(2):
                cut = pl.ds(k * half_w, half_w)
                wait_on(ring.at[slot, :, cut] if p < 3 else ring.at[slot, cut, :], ring_sem.at[slot, k])
        else:
            wait_on(ring.at[slot], ring_sem.at[slot, 0])

    half_n = seq_n // 2

    def place(p):
        return 2 * p + core, lax.rem(p, 2)

    def passed_on(p):
        seq, slot = place(p)
        return remote(inbox.at[p], hidden.at[seq], f_send.at[slot], st_recv.at[0, p], partner)

    def load_x(p):
        seq, slot = place(p)
        dst, sem = x_buf.at[slot], x_sem.at[slot]

        @pl.when(stage == 0)
        def _():
            pltpu.make_async_copy(x_hbm.at[seq], dst, sem).start()

        @pl.when(stage > 0)
        def _():
            wait_on(inbox.at[p], in_recv.at[p])

            @pl.when(is_odd & not_own)
            def _():
                pltpu.make_async_copy(hidden.at[seq], dst, sem).start()

            @pl.when(is_even | own)
            def _():
                pltpu.make_async_copy(inbox.at[p], dst, sem).start()

            @pl.when(is_odd & own)
            def _():
                pl.when(p >= 2)(lambda: passed_on(p - 2).wait_send())
                passed_on(p).start()

    def sends(p, src):
        seq, slot = place(p)
        return [
            (is_even & own, remote(src, hidden.at[seq], y_send.at[slot], in_recv.at[p], y_peer)),
            (is_even & not_own, remote(src, inbox.at[p], y_send.at[slot], in_recv.at[p], y_peer)),
            (is_odd, remote(src, hidden.at[seq], y_send.at[slot], st_recv.at[core, p], y_store)),
            (stage == 1, remote(src, inbox.at[p], x_send.at[slot], in_recv.at[p], x_peer)),
            (not_own, remote(src, hidden.at[seq], c_send.at[slot], st_recv.at[0, p], partner)),
        ]

    def each_send(p, what):
        @pl.when(own)
        def _():
            for cond, copy in sends(p, hidden.at[2 * p + core]):
                pl.when(cond)(functools.partial(what, copy))

        @pl.when(not_own)
        def _():
            for cond, copy in sends(p, ostage.at[p]):
                pl.when(cond)(functools.partial(what, copy))

    def store_out(p):
        pl.when(own)(lambda: pltpu.make_async_copy(out_buf, hidden.at[2 * p + core], l_sem).start())
        pl.when(not_own)(lambda: pltpu.make_async_copy(out_buf, ostage.at[p], l_sem).start())

    def start_sends(p):
        wait_on(out_buf, l_sem)
        pl.when(p >= 2)(lambda: each_send(p - 2, lambda copy: copy.wait_send()))
        each_send(p, lambda copy: copy.start())

    def wide(row):
        return jnp.concatenate([small[0, row:row + 1, :], small[0, row + 1:row + 2, :]], axis=-1)

    lane_tile = 128
    group_w = 384
    group_heads = group_w // head_dim
    groups_loc = heads_loc // group_heads
    spans = []
    for r in range(group_heads):
        low, high = r * head_dim, (r + 1) * head_dim
        start, stop = low // lane_tile * lane_tile, -(-high // lane_tile) * lane_tile
        spans.append((start, stop - start, low - start, high - start))
    q_rows = seq_n // 2
    sub = 16
    score_scale = head_dim ** -0.5 * LOG2E

    def scores(g):
        for qb in range(2):
            keys = (qb + 1) * q_rows
            for r, (start, span, low, high) in enumerate(spans):
                col = pl.ds(g * group_w + start, span)
                lane = lax.broadcasted_iota(jnp.int32, (keys, span), 1)
                k_val = qkv_buf[1, pl.ds(0, keys), col]
                k_val = jnp.where((lane >= low) & (lane < high), k_val, jnp.zeros_like(k_val))
                q_val = qkv_buf[0, pl.ds(qb * q_rows, q_rows), col]
                score_buf[qb, r, :, pl.ds(0, keys)] = lax.dot_general(q_val, k_val, (((1,), (1,)), ((), ())), preferred_element_type=F32)

    def soften(g):
        head = (y if g < groups_loc else 1 - y) * heads_loc + g % groups_loc * group_heads
        for qb in range(2):
            keys = (qb + 1) * q_rows
            for r in range(group_heads):
                slope = slopes[head + r]
                for blk in range(q_rows // sub):
                    rows = pl.ds(blk * sub, sub)
                    at = qb * q_rows + blk * sub
                    need = -(-(at + sub) // lane_tile) * lane_tile
                    score = score_buf[qb, r, rows, pl.ds(0, need)] * score_scale + slope * bias[pl.ds(at, sub), pl.ds(0, need)]
                    top = jnp.max(score, axis=-1, keepdims=True)
                    prob = jnp.exp2(score - top)
                    inv = 1.0 / jnp.sum(prob, axis=-1, keepdims=True)
                    prob_buf[qb, r, rows, pl.ds(0, need)] = (prob * inv).astype(BF16)
                    if need < keys:
                        prob_buf[qb, r, rows, pl.ds(need, keys - need)] = jnp.zeros((sub, keys - need), BF16)

    def contexts(g):
        lane = lax.broadcasted_iota(jnp.int32, (q_rows, lane_tile), 1)
        for qb in range(2):
            keys = (qb + 1) * q_rows
            outs = []
            for r, (start, span, low, high) in enumerate(spans):
                v_val = qkv_buf[2, pl.ds(0, keys), pl.ds(g * group_w + start, span)]
                outs.append(jnp.dot(prob_buf[qb, r, :, pl.ds(0, keys)], v_val, preferred_element_type=F32))
            for tile in range(group_w // lane_tile):
                value = None
                for r, (start, span, low, high) in enumerate(spans):
                    at = tile * lane_tile - start
                    if at < 0 or at >= span:
                        continue
                    piece = outs[r][:, at:at + lane_tile]
                    value = piece if value is None else jnp.where(lane >= low - at, piece, value)
                ctx_buf[pl.ds(qb * q_rows, q_rows), pl.ds(g * group_w + tile * lane_tile, lane_tile)] = value.astype(BF16)

    at_start = stage == 0

    @pl.when(stage > 0)
    def _():
        for j in range(pieces_n):
            arrive_a(j)
        for j in range(pieces_n):
            arrive_b(j)

    load_x(jnp.int32(0))
    for p in range(ring_n):
        load_tile(p, at_start)

    @pl.when(own)
    def _():
        small_local.wait()
        wait_on(small.at[1], small_sem.at[3])
        small_pass.start()

    @pl.when(not_own)
    def _():
        wait_on(small.at[0], small_sem.at[2])
        wait_on(small.at[1], small_sem.at[3])

    whole = pl.ds(0, seq_n)
    quarter_n = seq_n // 4
    two = [pl.ds(k * half_n, half_n) for k in range(2)]

    def one_unit(p, carry):
        seq, slot = place(p)
        first = at_start & (p == 0)
        more = p + 1 < units
        wait_on(x_buf.at[slot], x_sem.at[slot])
        length = lens[seq // lens.shape[1], lax.rem(seq, lens.shape[1])]

        def position_bias():
            block = 64
            for rows in range(0, seq_n, block):
                query_pos = rows + lax.broadcasted_iota(jnp.int32, (block, seq_n), 0)
                key_pos = lax.broadcasted_iota(jnp.int32, (block, seq_n), 1)
                allowed = (key_pos <= query_pos) & (key_pos < length)
                bias[rows:rows + block, :] = jnp.where(allowed, (key_pos - query_pos).astype(F32), MASKED)

        gain1, shift1 = wide(LN1_G), wide(LN1_S)

        def first_norm(low):
            for at in range(low, low + quarter_n, 16):
                a_buf[at:at + 16, :] = normalize(x_buf[slot, at:at + 16, :].astype(F32), gain1, shift1)

        def project(j, start, size, rows=whole):
            both = jnp.concatenate([small[k, B_QKV + j:B_QKV + j + 1, :] for k in range(2)], axis=-1)
            value = jnp.dot(a_buf[rows, :], ring[j, :, pl.ds(start, size)], preferred_element_type=F32)
            qkv_buf[j, rows, pl.ds(start, size)] = (value + both[:, start:start + size]).astype(BF16)

        def out_part(k_low, k_size, low, size):
            part = pl.ds(k_low, k_size)
            acc[:, pl.ds(low, size)] = jnp.dot(ctx_buf[:, part], ring[3, part, pl.ds(low, size)], preferred_element_type=F32)

        bias_out, bias_down, gain2, shift2 = wide(B_OUT), wide(B_DOWN), wide(LN2_G), wide(LN2_S)

        def add_attended(rows):
            resid = (x_buf[slot, rows, :].astype(F32) + acc[rows, :] + jnp.dot(ctx_buf[rows, half_w:], ring[3, half_w:, :], preferred_element_type=F32) + bias_out).astype(BF16)
            h_buf[rows, :] = resid
            acc[rows, :] = resid.astype(F32) + bias_down

        def second_norm(low):
            for at in range(low, low + half_n, 16):
                a_buf[at:at + 16, :] = normalize(h_buf[at:at + 16, :].astype(F32), gain2, shift2)

        def up(m, rows=whole):
            row = B_UP + 2 * lax.rem(m, parts)
            part = m // parts
            both = jnp.concatenate([small[part, pl.ds(row + k, 1), :] for k in range(2)], axis=-1)
            value = jnp.dot(a_buf[rows, :], ring[2 * lax.rem(m, 2)], preferred_element_type=F32) + both
            u_buf[lax.rem(m, 2), rows, :] = gelu(value).astype(BF16)

        def down(m):
            return jnp.dot(u_buf[lax.rem(m, 2)], ring[2 * lax.rem(m, 2) + 1], preferred_element_type=F32)

        cut = 2 * width // 3
        first_norm(0)
        pl.when(p > 0)(lambda: start_sends(p - 1))
        pl.when((stage == 0) & own & (p == 1))(lambda: pass_on(pieces_n - 1).start())
        pl.when(p == 0)(lambda: wait_tile(0))
        for j in (1, 2):
            wait_tile(j)
        for low in range(0, seq_n, quarter_n):
            project(0, 0, cut, pl.ds(low, quarter_n))
            if low + quarter_n < seq_n:
                first_norm(low + quarter_n)
        position_bias()
        project(1, 0, cut)
        project(2, 0, cut)
        scores(0)
        project(0, cut, width - cut)
        soften(0)
        scores(1)
        contexts(0)
        project(1, cut, width - cut)
        soften(1)
        project(2, cut, width - cut)
        contexts(1)
        for t in (4, 5, 6):
            load_tile(t, first)
        for t in (3, 4):
            wait_tile(t)
        scores(2)
        out_part(0, half_w, 0, cut)
        soften(2)
        scores(3)
        contexts(2)
        out_part(0, half_w, cut, width - cut)
        soften(3)
        contexts(3)
        for rows in two:
            add_attended(rows)
        second_norm(0)
        up(0, two[0])
        second_norm(half_n)
        up(0, two[1])
        load_tile(7, first)
        load_tile(8, first)

        def mlp(m, carry):
            up_slot, down_slot = 2 * lax.rem(m + 1, 2), 2 * lax.rem(m, 2) + 1
            wait_on(ring.at[up_slot], ring_sem.at[up_slot, 0])
            wait_on(ring.at[down_slot], ring_sem.at[down_slot, 0])
            up(m + 1)
            acc[...] += down(m)
            for at in range(chunks - 1):
                @pl.when(m == at)
                def _(at=at):
                    for t in (10 + 2 * at, 9 + 2 * at):
                        if t < tiles_n:
                            load_tile(t, first)
                        else:
                            pl.when(more)(functools.partial(load_tile, t))
            return carry

        lax.fori_loop(0, chunks - 1, mlp, 0)
        pl.when(more)(lambda: load_x(p + 1))
        wait_tile(11)
        pl.when(more)(lambda: wait_tile(0))
        out_buf[...] = (acc[...] + down(chunks - 1)).astype(BF16)
        pl.when(more)(functools.partial(load_tile, tiles_n + 3))
        store_out(p)
        return carry

    lax.fori_loop(0, units, one_unit, 0)
    start_sends(jnp.int32(units - 1))

    def settle(n, carry):
        p = units - 2 + n
        each_send(p, lambda copy: copy.wait_send())
        pl.when(is_odd & own)(lambda: passed_on(p).wait_send())
        return carry

    lax.fori_loop(0, 2, settle, 0)

    for j in range(pieces_n):
        wait_on(mine[j], w_send.at[j])
        pl.when(own)(lambda j=j: pass_on(j).wait_send())
    wait_on(small_hbm, small_sem.at[1])
    pl.when(own)(lambda: small_pass.wait_send())

    def drain(p, carry):
        wait_on(hidden.at[p], st_recv.at[0, p])
        pl.when(is_even & not_own)(lambda: wait_on(hidden.at[p], st_recv.at[1, p]))
        return carry

    lax.fori_loop(0, units, drain, 0)


def solution(mesh):
    in_specs = (P('dp'), P('dp'), P('pp'), P('pp'), P('pp', None, None, 'tp'), P('pp', None, 'tp', None), P('pp', 'tp', None), P('pp'), P('pp'), P('pp'), P('pp', None, 'tp'), P('pp', 'tp'), P('pp', 'tp', None), P('pp'))

    def per_device(x_in, seq_lens, ln1_gain, ln1_shift, w_qkv, b_qkv, w_out, b_out, ln2_gain, ln2_shift, w_up, b_up, w_down, b_down):
        micro_n, batch_n, seq_n, width = x_in.shape
        total = micro_n * batch_n
        units = total // 2
        half_w = w_out.shape[1]
        head_dim = b_qkv.shape[3]
        heads_n = width // head_dim
        up_w = w_up.shape[2]
        parts = up_w // width
        rows_n = (6 * width + 3 * half_w + up_w) // half_w
        packed = pl.pallas_call(
            pack_kernel,
            out_shape=jax.ShapeDtypeStruct((rows_n + -rows_n % 8, half_w), F32),
            name='pack_kernel',
        )(ln1_gain, ln1_shift, b_out, ln2_gain, ln2_shift, b_down, b_qkv.reshape(1, -1), b_up)
        slopes = jnp.asarray(np.array(alibi_slopes(heads_n), np.float32) * np.float32(LOG2E))
        wqkv = jnp.transpose(w_qkv[0], (1, 0, 2))
        weights = (wqkv, w_out[0], w_up[0], w_down[0])
        hbm = pl.BlockSpec(memory_space=pl.ANY)
        smem = pl.BlockSpec(memory_space=pltpu.SMEM)
        seq_t = lambda n: jax.ShapeDtypeStruct((n, seq_n, width), BF16)
        half_t = [
            jax.ShapeDtypeStruct(wqkv.shape, BF16),
            jax.ShapeDtypeStruct((half_w, width), BF16),
            jax.ShapeDtypeStruct((parts, width, width), BF16),
            jax.ShapeDtypeStruct((up_w, width), BF16),
        ]
        pieces_n = 4 + 2 * parts
        flops = 2 * units * seq_n * width * (4 * width + 4 * up_w)
        outs = pl.pallas_call(
            functools.partial(stage_kernel, units, head_dim),
            out_shape=[seq_t(total), seq_t(units), seq_t(units)] + half_t + half_t,
            in_specs=[hbm, smem, smem, hbm] + [hbm] * 4,
            out_specs=[hbm] * 11,
            scratch_shapes=[
                pltpu.VMEM((2,) + packed.shape, F32),
                pltpu.VMEM((2, seq_n, width), BF16),
                pltpu.VMEM((seq_n, width), BF16),
                pltpu.VMEM((3, seq_n, width), BF16),
                pltpu.VMEM((seq_n, width), BF16),
                pltpu.VMEM((seq_n, width), BF16),
                pltpu.VMEM((seq_n, width), F32),
                pltpu.VMEM((2, seq_n, width), BF16),
                pltpu.VMEM((seq_n, seq_n), F32),
                pltpu.VMEM((2, 4, seq_n // 2, seq_n), F32),
                pltpu.VMEM((2, 4, seq_n // 2, seq_n), BF16),
                pltpu.VMEM((seq_n, width), BF16),
                pltpu.VMEM((4, width, width), BF16),
                pltpu.SemaphoreType.DMA((5,)),
                pltpu.SemaphoreType.DMA((pieces_n,)),
                pltpu.SemaphoreType.DMA((pieces_n,)),
                pltpu.SemaphoreType.DMA((pieces_n,)),
                pltpu.SemaphoreType.DMA((pieces_n,)),
                pltpu.SemaphoreType.DMA((units,)),
                pltpu.SemaphoreType.DMA((2, units)),
                pltpu.SemaphoreType.DMA((4, 2)),
                pltpu.SemaphoreType.DMA((2,)),
                pltpu.SemaphoreType.DMA,
                pltpu.SemaphoreType.DMA((2,)),
                pltpu.SemaphoreType.DMA((2,)),
                pltpu.SemaphoreType.DMA((2,)),
                pltpu.SemaphoreType.DMA((2,)),
            ],
            compiler_params=pltpu.CompilerParams(collective_id=0, has_side_effects=True, vmem_limit_bytes=63 * 1024 * 1024),
            cost_estimate=pl.CostEstimate(flops=flops, bytes_accessed=1 << 31, transcendentals=0),
            name='stage_kernel',
        )(x_in.reshape(total, seq_n, width), seq_lens, slopes, packed, *weights)
        return outs[0].reshape((1,) + x_in.shape)

    return jax.shard_map(per_device, mesh=mesh, in_specs=in_specs, out_specs=P('pp', 'dp'), check_vma=False)
```

```python
import functools
import math

import jax
import jax.numpy as jnp
import numpy as np
from jax import lax
from jax.experimental import pallas as pl
from jax.experimental.pallas import tpu as pltpu
from jax.sharding import PartitionSpec as P

MESH = pl.DeviceIdType.MESH
LOG2E = math.log2(math.e)
MASKED = -1e34
F32 = jnp.float32
BF16 = jnp.bfloat16
LN1_G, LN1_S, B_OUT, LN2_G, LN2_S, B_DOWN, B_QKV, B_UP = 0, 2, 4, 6, 8, 10, 12, 15


def alibi_slopes(heads_n):
    closest = 2 ** int(math.floor(math.log2(heads_n)))
    base_rate = 2.0 ** (-8.0 / closest)
    slope_list = [base_rate ** (head_idx + 1) for head_idx in range(closest)]
    extra_rate = 2.0 ** (-4.0 / closest)
    return slope_list + [extra_rate ** (2 * head_idx + 1) for head_idx in range(min(closest, heads_n - closest))]


def normalize(val_f, gain, shift):
    width = val_f.shape[-1]
    mean_val = jnp.sum(val_f, axis=-1, keepdims=True) * (1.0 / width)
    centered = val_f - mean_val
    var_val = jnp.sum(centered * centered, axis=-1, keepdims=True) * (1.0 / width)
    normed = centered * lax.rsqrt(var_val + 1e-5)
    return (normed * gain + shift).astype(BF16)


def gelu(val):
    inner = val * (0.7978845608028654 + (0.7978845608028654 * 0.044715) * (val * val))
    half = 0.5 * val
    return half + half * jnp.tanh(inner)


def pack_kernel(*refs):
    packed = refs[-1]
    wide = packed.shape[1]
    row = 0
    for ref in refs[:-1]:
        for low in range(0, ref.shape[1], wide):
            packed[row:row + 1, :] = ref[0:1, low:low + wide].astype(F32)
            row += 1
    packed[row:, :] = jnp.zeros((packed.shape[0] - row, wide), F32)


def stage_kernel(
    units, head_dim,
    x_hbm, lens, slopes, small_hbm, wqkv, wout, wup, wdown,
    hidden, inbox, ostage, wa_qkv, wa_out, wa_up, wa_down, wb_qkv, wb_out, wb_up, wb_down,
    small, x_buf, a_buf, qkv_buf, ctx_buf, h_buf, acc, u_buf, bias, score_buf, prob_buf, out_buf, ring,
    small_sem, wa_recv, wb_recv, w_send, w_fwd, in_recv, st_recv, ring_sem, x_sem, l_sem,
    y_send, c_send, x_send, f_send,
):
    dp = lax.axis_index('dp')
    y = lax.axis_index('tp')
    pp = lax.axis_index('pp')
    core = lax.rem(pp, 2)
    chip_x = pp // 2
    odd = lax.rem(chip_x + y, 2)
    stage = 2 * chip_x + odd
    own = core == odd
    not_own = core != odd
    is_odd = odd == 1
    is_even = odd == 0
    partner = (dp, y, 2 * chip_x + 1 - core)
    y_peer = (dp, 1 - y, pp)
    y_store = (dp, 1 - y, 2 * chip_x + 1)
    y_other = (dp, 1 - y, 2 * chip_x + 1 - core)
    x_peer = (dp, y, lax.rem(pp + 2, 4))
    seq_n, width = a_buf.shape
    half_w = wout.shape[0]
    heads_loc = half_w // head_dim
    parts = wup.shape[1] // width
    chunks = 2 * parts

    barrier = pltpu.get_barrier_semaphore()
    for other in (partner, y_peer, y_other, x_peer):
        pl.semaphore_signal(barrier, inc=1, device_id=other, device_id_type=MESH)
    pl.semaphore_wait(barrier, 4)

    def remote(src, dst, send_sem, recv_sem, device):
        return pltpu.make_async_remote_copy(src_ref=src, dst_ref=dst, send_sem=send_sem, recv_sem=recv_sem, device_id=device, device_id_type=MESH)

    def wait_on(ref, sem):
        pltpu.make_async_copy(ref, ref, sem).wait()

    def pieces(qkv, out, up, down, up_cut):
        found = [qkv.at[j] for j in range(3)] + [out]
        for m in range(parts):
            found.append(up.at[:, pl.ds(m * width, width)] if up_cut else up.at[m])
            found.append(down.at[pl.ds(m * width, width), :])
        return found

    mine = pieces(wqkv, wout, wup, wdown, True)
    got_a = pieces(wa_qkv, wa_out, wa_up, wa_down, False)
    got_b = pieces(wb_qkv, wb_out, wb_up, wb_down, False)
    pieces_n = len(mine)

    small_local = pltpu.make_async_copy(small_hbm, small.at[0], small_sem.at[0])
    small_give = remote(small_hbm, small.at[0], small_sem.at[1], small_sem.at[2], partner)
    small_cross = remote(small_hbm, small.at[1], small_sem.at[1], small_sem.at[3], y_peer)
    small_pass = remote(small.at[1], small.at[1], small_sem.at[4], small_sem.at[3], partner)

    @pl.when(own)
    def _():
        small_local.start()
        small_give.start()
        for j in range(pieces_n):
            remote(mine[j], got_a[j], w_send.at[j], wa_recv.at[j], partner).start()

    @pl.when(not_own)
    def _():
        small_cross.start()
        for j in range(pieces_n):
            remote(mine[j], got_b[j], w_send.at[j], wb_recv.at[j], y_peer).start()

    def pass_on(j):
        return remote(got_b[j], got_b[j], w_fwd.at[j], wb_recv.at[j], partner)

    def arrive_a(j):
        pl.when(not_own)(lambda: wait_on(got_a[j], wa_recv.at[j]))

    def arrive_b(j):
        wait_on(got_b[j], wb_recv.at[j])
        pl.when(own if j < pieces_n - 1 else own & (stage > 0))(lambda: pass_on(j).start())

    def copy_a(j, dst, sem):
        pl.when(own)(lambda: pltpu.make_async_copy(mine[j], dst, sem).start())
        pl.when(not_own)(lambda: pltpu.make_async_copy(got_a[j], dst, sem).start())

    def copy_b(j, dst, sem):
        pltpu.make_async_copy(got_b[j], dst, sem).start()

    tiles_n = 4 + 2 * chunks
    ring_n = ring.shape[0]

    def load_tile(p, first=None):
        p = p % tiles_n
        slot = p % ring_n
        if p < 4:
            left = ring.at[slot, :, pl.ds(0, half_w)] if p < 3 else ring.at[slot, pl.ds(0, half_w), :]
            right = ring.at[slot, :, pl.ds(half_w, half_w)] if p < 3 else ring.at[slot, pl.ds(half_w, half_w), :]
            if first is not None:
                @pl.when(first)
                def _():
                    arrive_a(p)
                    arrive_b(p)
            copy_a(p, left, ring_sem.at[slot, 0])
            copy_b(p, right, ring_sem.at[slot, 1])
        else:
            m, is_down = (p - 4) // 2, (p - 4) % 2
            j = 4 + 2 * (m % parts) + is_down
            arrive, copy = (arrive_a, copy_a) if m < parts else (arrive_b, copy_b)
            if first is not None:
                pl.when(first)(lambda: arrive(j))
            copy(j, ring.at[slot], ring_sem.at[slot, 0])

    def wait_tile(p):
        slot = p % ring_n
        if p < 4:
            for k in range(2):
                cut = pl.ds(k * half_w, half_w)
                wait_on(ring.at[slot, :, cut] if p < 3 else ring.at[slot, cut, :], ring_sem.at[slot, k])
        else:
            wait_on(ring.at[slot], ring_sem.at[slot, 0])

    half_n = seq_n // 2

    def place(p):
        return 2 * p + core, lax.rem(p, 2)

    def passed_on(p):
        seq, slot = place(p)
        return remote(inbox.at[p], hidden.at[seq], f_send.at[slot], st_recv.at[0, p], partner)

    def load_x(p):
        seq, slot = place(p)
        dst, sem = x_buf.at[slot], x_sem.at[slot]

        @pl.when(stage == 0)
        def _():
            pltpu.make_async_copy(x_hbm.at[seq], dst, sem).start()

        @pl.when(stage > 0)
        def _():
            wait_on(inbox.at[p], in_recv.at[p])

            @pl.when(is_odd & not_own)
            def _():
                pltpu.make_async_copy(hidden.at[seq], dst, sem).start()

            @pl.when(is_even | own)
            def _():
                pltpu.make_async_copy(inbox.at[p], dst, sem).start()

            @pl.when(is_odd & own)
            def _():
                pl.when(p >= 2)(lambda: passed_on(p - 2).wait_send())
                passed_on(p).start()

    def sends(p, src):
        seq, slot = place(p)
        return [
            (is_even & own, remote(src, hidden.at[seq], y_send.at[slot], in_recv.at[p], y_peer)),
            (is_even & not_own, remote(src, inbox.at[p], y_send.at[slot], in_recv.at[p], y_peer)),
            (is_odd, remote(src, hidden.at[seq], y_send.at[slot], st_recv.at[core, p], y_store)),
            (stage == 1, remote(src, inbox.at[p], x_send.at[slot], in_recv.at[p], x_peer)),
            (not_own, remote(src, hidden.at[seq], c_send.at[slot], st_recv.at[0, p], partner)),
        ]

    def each_send(p, what):
        @pl.when(own)
        def _():
            for cond, copy in sends(p, hidden.at[2 * p + core]):
                pl.when(cond)(functools.partial(what, copy))

        @pl.when(not_own)
        def _():
            for cond, copy in sends(p, ostage.at[p]):
                pl.when(cond)(functools.partial(what, copy))

    def store_out(p):
        pl.when(own)(lambda: pltpu.make_async_copy(out_buf, hidden.at[2 * p + core], l_sem).start())
        pl.when(not_own)(lambda: pltpu.make_async_copy(out_buf, ostage.at[p], l_sem).start())

    def start_sends(p):
        wait_on(out_buf, l_sem)
        pl.when(p >= 2)(lambda: each_send(p - 2, lambda copy: copy.wait_send()))
        each_send(p, lambda copy: copy.start())

    def wide(row):
        return jnp.concatenate([small[0, row:row + 1, :], small[0, row + 1:row + 2, :]], axis=-1)

    lane_tile = 128
    group_w = 384
    group_heads = group_w // head_dim
    groups_loc = heads_loc // group_heads
    spans = []
    for r in range(group_heads):
        low, high = r * head_dim, (r + 1) * head_dim
        start, stop = low // lane_tile * lane_tile, -(-high // lane_tile) * lane_tile
        spans.append((start, stop - start, low - start, high - start))
    q_rows = seq_n // 2
    sub = 16
    score_scale = head_dim ** -0.5 * LOG2E

    def scores(g):
        for qb in range(2):
            keys = (qb + 1) * q_rows
            for r, (start, span, low, high) in enumerate(spans):
                col = pl.ds(g * group_w + start, span)
                lane = lax.broadcasted_iota(jnp.int32, (keys, span), 1)
                k_val = qkv_buf[1, pl.ds(0, keys), col]
                k_val = jnp.where((lane >= low) & (lane < high), k_val, jnp.zeros_like(k_val))
                q_val = qkv_buf[0, pl.ds(qb * q_rows, q_rows), col]
                score_buf[qb, r, :, pl.ds(0, keys)] = lax.dot_general(q_val, k_val, (((1,), (1,)), ((), ())), preferred_element_type=F32)

    def soften(g):
        head = (y if g < groups_loc else 1 - y) * heads_loc + g % groups_loc * group_heads
        for qb in range(2):
            keys = (qb + 1) * q_rows
            for r in range(group_heads):
                slope = slopes[head + r]
                for blk in range(q_rows // sub):
                    rows = pl.ds(blk * sub, sub)
                    at = qb * q_rows + blk * sub
                    need = -(-(at + sub) // lane_tile) * lane_tile
                    score = score_buf[qb, r, rows, pl.ds(0, need)] * score_scale + slope * bias[pl.ds(at, sub), pl.ds(0, need)]
                    top = jnp.max(score, axis=-1, keepdims=True)
                    prob = jnp.exp2(score - top)
                    inv = 1.0 / jnp.sum(prob, axis=-1, keepdims=True)
                    prob_buf[qb, r, rows, pl.ds(0, need)] = (prob * inv).astype(BF16)
                    if need < keys:
                        prob_buf[qb, r, rows, pl.ds(need, keys - need)] = jnp.zeros((sub, keys - need), BF16)

    def contexts(g):
        lane = lax.broadcasted_iota(jnp.int32, (q_rows, lane_tile), 1)
        for qb in range(2):
            keys = (qb + 1) * q_rows
            outs = []
            for r, (start, span, low, high) in enumerate(spans):
                v_val = qkv_buf[2, pl.ds(0, keys), pl.ds(g * group_w + start, span)]
                outs.append(jnp.dot(prob_buf[qb, r, :, pl.ds(0, keys)], v_val, preferred_element_type=F32))
            for tile in range(group_w // lane_tile):
                value = None
                for r, (start, span, low, high) in enumerate(spans):
                    at = tile * lane_tile - start
                    if at < 0 or at >= span:
                        continue
                    piece = outs[r][:, at:at + lane_tile]
                    value = piece if value is None else jnp.where(lane >= low - at, piece, value)
                ctx_buf[pl.ds(qb * q_rows, q_rows), pl.ds(g * group_w + tile * lane_tile, lane_tile)] = value.astype(BF16)

    at_start = stage == 0

    @pl.when(stage > 0)
    def _():
        for j in range(pieces_n):
            arrive_a(j)
        for j in range(pieces_n):
            arrive_b(j)

    load_x(jnp.int32(0))
    for p in range(ring_n):
        load_tile(p, at_start)

    @pl.when(own)
    def _():
        small_local.wait()
        wait_on(small.at[1], small_sem.at[3])
        small_pass.start()

    @pl.when(not_own)
    def _():
        wait_on(small.at[0], small_sem.at[2])
        wait_on(small.at[1], small_sem.at[3])

    whole = pl.ds(0, seq_n)
    quarter_n = seq_n // 4
    two = [pl.ds(k * half_n, half_n) for k in range(2)]

    def one_unit(p, carry):
        seq, slot = place(p)
        first = at_start & (p == 0)
        more = p + 1 < units
        wait_on(x_buf.at[slot], x_sem.at[slot])
        length = lens[seq // lens.shape[1], lax.rem(seq, lens.shape[1])]

        def position_bias():
            block = 64
            for rows in range(0, seq_n, block):
                query_pos = rows + lax.broadcasted_iota(jnp.int32, (block, seq_n), 0)
                key_pos = lax.broadcasted_iota(jnp.int32, (block, seq_n), 1)
                allowed = (key_pos <= query_pos) & (key_pos < length)
                bias[rows:rows + block, :] = jnp.where(allowed, (key_pos - query_pos).astype(F32), MASKED)

        gain1, shift1 = wide(LN1_G), wide(LN1_S)

        def first_norm(low):
            for at in range(low, low + quarter_n, 16):
                a_buf[at:at + 16, :] = normalize(x_buf[slot, at:at + 16, :].astype(F32), gain1, shift1)

        def project(j, start, size, rows=whole):
            both = jnp.concatenate([small[k, B_QKV + j:B_QKV + j + 1, :] for k in range(2)], axis=-1)
            value = jnp.dot(a_buf[rows, :], ring[j, :, pl.ds(start, size)], preferred_element_type=F32)
            qkv_buf[j, rows, pl.ds(start, size)] = (value + both[:, start:start + size]).astype(BF16)

        def out_part(k_low, k_size, low, size):
            part = pl.ds(k_low, k_size)
            acc[:, pl.ds(low, size)] = jnp.dot(ctx_buf[:, part], ring[3, part, pl.ds(low, size)], preferred_element_type=F32)

        bias_out, bias_down, gain2, shift2 = wide(B_OUT), wide(B_DOWN), wide(LN2_G), wide(LN2_S)

        def add_attended(rows):
            resid = (x_buf[slot, rows, :].astype(F32) + acc[rows, :] + jnp.dot(ctx_buf[rows, half_w:], ring[3, half_w:, :], preferred_element_type=F32) + bias_out).astype(BF16)
            h_buf[rows, :] = resid
            acc[rows, :] = resid.astype(F32) + bias_down

        def second_norm(low):
            for at in range(low, low + half_n, 16):
                a_buf[at:at + 16, :] = normalize(h_buf[at:at + 16, :].astype(F32), gain2, shift2)

        def up(m, rows=whole):
            row = B_UP + 2 * lax.rem(m, parts)
            part = m // parts
            both = jnp.concatenate([small[part, pl.ds(row + k, 1), :] for k in range(2)], axis=-1)
            value = jnp.dot(a_buf[rows, :], ring[2 * lax.rem(m, 2)], preferred_element_type=F32) + both
            u_buf[lax.rem(m, 2), rows, :] = gelu(value).astype(BF16)

        def down(m):
            return jnp.dot(u_buf[lax.rem(m, 2)], ring[2 * lax.rem(m, 2) + 1], preferred_element_type=F32)

        cut = 2 * width // 3
        first_norm(0)
        pl.when(p > 0)(lambda: start_sends(p - 1))
        pl.when(p == 0)(lambda: wait_tile(0))
        for j in (1, 2):
            wait_tile(j)
        for low in range(0, seq_n, quarter_n):
            project(0, 0, cut, pl.ds(low, quarter_n))
            if low + quarter_n < seq_n:
                first_norm(low + quarter_n)
        position_bias()
        project(1, 0, cut)
        project(2, 0, cut)
        scores(0)
        project(0, cut, width - cut)
        soften(0)
        scores(1)
        contexts(0)
        project(1, cut, width - cut)
        soften(1)
        project(2, cut, width - cut)
        contexts(1)
        for t in (4, 5, 6):
            load_tile(t, first)
        pl.when((stage == 0) & own & (p == 1))(lambda: pass_on(pieces_n - 1).start())
        for t in (3, 4):
            wait_tile(t)
        scores(2)
        out_part(0, half_w, 0, cut)
        soften(2)
        scores(3)
        contexts(2)
        out_part(0, half_w, cut, width - cut)
        soften(3)
        contexts(3)
        for rows in two:
            add_attended(rows)
        second_norm(0)
        up(0, two[0])
        second_norm(half_n)
        up(0, two[1])
        load_tile(7, first)
        load_tile(8, first)

        def mlp(m, carry):
            up_slot, down_slot = 2 * lax.rem(m + 1, 2), 2 * lax.rem(m, 2) + 1
            wait_on(ring.at[up_slot], ring_sem.at[up_slot, 0])
            wait_on(ring.at[down_slot], ring_sem.at[down_slot, 0])
            up(m + 1)
            acc[...] += down(m)
            for at in range(chunks - 1):
                @pl.when(m == at)
                def _(at=at):
                    for t in (10 + 2 * at, 9 + 2 * at):
                        if t < tiles_n:
                            load_tile(t, first)
                        else:
                            pl.when(more)(functools.partial(load_tile, t))
            return carry

        lax.fori_loop(0, chunks - 1, mlp, 0)
        pl.when(more)(lambda: load_x(p + 1))
        wait_tile(11)
        pl.when(more)(lambda: wait_tile(0))
        out_buf[...] = (acc[...] + down(chunks - 1)).astype(BF16)
        pl.when(more)(functools.partial(load_tile, tiles_n + 3))
        store_out(p)
        return carry

    lax.fori_loop(0, units, one_unit, 0)
    start_sends(jnp.int32(units - 1))

    def settle(n, carry):
        p = units - 2 + n
        each_send(p, lambda copy: copy.wait_send())
        pl.when(is_odd & own)(lambda: passed_on(p).wait_send())
        return carry

    lax.fori_loop(0, 2, settle, 0)

    for j in range(pieces_n):
        wait_on(mine[j], w_send.at[j])
        pl.when(own)(lambda j=j: pass_on(j).wait_send())
    wait_on(small_hbm, small_sem.at[1])
    pl.when(own)(lambda: small_pass.wait_send())

    def drain(p, carry):
        wait_on(hidden.at[p], st_recv.at[0, p])
        pl.when(is_even & not_own)(lambda: wait_on(hidden.at[p], st_recv.at[1, p]))
        return carry

    lax.fori_loop(0, units, drain, 0)


def solution(mesh):
    in_specs = (P('dp'), P('dp'), P('pp'), P('pp'), P('pp', None, None, 'tp'), P('pp', None, 'tp', None), P('pp', 'tp', None), P('pp'), P('pp'), P('pp'), P('pp', None, 'tp'), P('pp', 'tp'), P('pp', 'tp', None), P('pp'))

    def per_device(x_in, seq_lens, ln1_gain, ln1_shift, w_qkv, b_qkv, w_out, b_out, ln2_gain, ln2_shift, w_up, b_up, w_down, b_down):
        micro_n, batch_n, seq_n, width = x_in.shape
        total = micro_n * batch_n
        units = total // 2
        half_w = w_out.shape[1]
        head_dim = b_qkv.shape[3]
        heads_n = width // head_dim
        up_w = w_up.shape[2]
        parts = up_w // width
        rows_n = (6 * width + 3 * half_w + up_w) // half_w
        packed = pl.pallas_call(
            pack_kernel,
            out_shape=jax.ShapeDtypeStruct((rows_n + -rows_n % 8, half_w), F32),
            name='pack_kernel',
        )(ln1_gain, ln1_shift, b_out, ln2_gain, ln2_shift, b_down, b_qkv.reshape(1, -1), b_up)
        slopes = jnp.asarray(np.array(alibi_slopes(heads_n), np.float32) * np.float32(LOG2E))
        wqkv = jnp.transpose(w_qkv[0], (1, 0, 2))
        weights = (wqkv, w_out[0], w_up[0], w_down[0])
        hbm = pl.BlockSpec(memory_space=pl.ANY)
        smem = pl.BlockSpec(memory_space=pltpu.SMEM)
        seq_t = lambda n: jax.ShapeDtypeStruct((n, seq_n, width), BF16)
        half_t = [
            jax.ShapeDtypeStruct(wqkv.shape, BF16),
            jax.ShapeDtypeStruct((half_w, width), BF16),
            jax.ShapeDtypeStruct((parts, width, width), BF16),
            jax.ShapeDtypeStruct((up_w, width), BF16),
        ]
        pieces_n = 4 + 2 * parts
        flops = 2 * units * seq_n * width * (4 * width + 4 * up_w)
        outs = pl.pallas_call(
            functools.partial(stage_kernel, units, head_dim),
            out_shape=[seq_t(total), seq_t(units), seq_t(units)] + half_t + half_t,
            in_specs=[hbm, smem, smem, hbm] + [hbm] * 4,
            out_specs=[hbm] * 11,
            scratch_shapes=[
                pltpu.VMEM((2,) + packed.shape, F32),
                pltpu.VMEM((2, seq_n, width), BF16),
                pltpu.VMEM((seq_n, width), BF16),
                pltpu.VMEM((3, seq_n, width), BF16),
                pltpu.VMEM((seq_n, width), BF16),
                pltpu.VMEM((seq_n, width), BF16),
                pltpu.VMEM((seq_n, width), F32),
                pltpu.VMEM((2, seq_n, width), BF16),
                pltpu.VMEM((seq_n, seq_n), F32),
                pltpu.VMEM((2, 4, seq_n // 2, seq_n), F32),
                pltpu.VMEM((2, 4, seq_n // 2, seq_n), BF16),
                pltpu.VMEM((seq_n, width), BF16),
                pltpu.VMEM((4, width, width), BF16),
                pltpu.SemaphoreType.DMA((5,)),
                pltpu.SemaphoreType.DMA((pieces_n,)),
                pltpu.SemaphoreType.DMA((pieces_n,)),
                pltpu.SemaphoreType.DMA((pieces_n,)),
                pltpu.SemaphoreType.DMA((pieces_n,)),
                pltpu.SemaphoreType.DMA((units,)),
                pltpu.SemaphoreType.DMA((2, units)),
                pltpu.SemaphoreType.DMA((4, 2)),
                pltpu.SemaphoreType.DMA((2,)),
                pltpu.SemaphoreType.DMA,
                pltpu.SemaphoreType.DMA((2,)),
                pltpu.SemaphoreType.DMA((2,)),
                pltpu.SemaphoreType.DMA((2,)),
                pltpu.SemaphoreType.DMA((2,)),
            ],
            compiler_params=pltpu.CompilerParams(collective_id=0, has_side_effects=True, vmem_limit_bytes=63 * 1024 * 1024),
            cost_estimate=pl.CostEstimate(flops=flops, bytes_accessed=1 << 31, transcendentals=0),
            name='stage_kernel',
        )(x_in.reshape(total, seq_n, width), seq_lens, slopes, packed, *weights)
        return outs[0].reshape((1,) + x_in.shape)

    return jax.shard_map(per_device, mesh=mesh, in_specs=in_specs, out_specs=P('pp', 'dp'), check_vma=False)
```
